128 devices in a mesh: rep: 1, dp: 128 (over x, y, z, core).
Axes of the slice: x: 4, y: 4, z: 4, core: 2. Of those that a mesh axis runs over, the one named last changes fastest.
Arguments:
- x: bfloat16 [128, 2048, 896], P(('rep', 'dp'))
- dy: bfloat16 [128, 2048, 896], P(('rep', 'dp'))
- w_gate: bfloat16 [2, 896, 2304], P(None, 'dp')
- w_up: bfloat16 [2, 896, 2304], P(None, 'dp')
- w_down: bfloat16 [2, 2304, 896], P(None, 'dp')
Outputs:
- output 1: bfloat16 [128, 2048, 896], P(('rep', 'dp'))
- output 2: bfloat16 [2, 896, 2304], P('rep', 'dp')
- output 3: bfloat16 [2, 896, 2304], P('rep', 'dp')
- output 4: bfloat16 [2, 2304, 896], P('rep', 'dp')
All inputs are finite; a program needn't handle non-finite values.
Results may differ from the reference program's by a relative error of at most 0.018.
Values are sent between devices in bfloat16 or wider.
A program may use at most 1.5 GiB of HBM per device.

```python
import jax
import jax.numpy as jnp
from jax import lax

SEQUENCES = 128
TOKENS = 2048
D = 896
FF = 2304
LAYERS = 2
NAMES = ("w_gate", "w_up", "w_down")
SHAPES = {"w_gate": (LAYERS, D, FF), "w_up": (LAYERS, D, FF), "w_down": (LAYERS, FF, D)}


def bump(key, n, height):
    away = (jnp.arange(n, dtype=jnp.int32) - jax.random.randint(key, (), 0, n, jnp.int32)) % n
    return jnp.where(away < n // 8, height, 1.0)


def together(key, own, strength):
    shared = jax.random.normal(key, own.shape[1:], jnp.float32)
    return (own + strength * shared) * lax.rsqrt(1 + strength * strength)


def setup_inputs(seed: int = 0, part: int = 0) -> dict:
    kx, kdy, ka, kb, kz, kf, kh, kl, *kw = jax.random.split(jax.random.key(seed), 8 + len(NAMES))
    kx, kdy, ka, kb = (jax.random.fold_in(k, part) for k in (kx, kdy, ka, kb))
    shape = (SEQUENCES, TOKENS, D)
    much_x, much_dy = jax.random.uniform(kz, (2,), jnp.float32, 0.0, 1.0)
    layers = 2.0 ** jax.random.uniform(kl, (LAYERS, 1, 1), jnp.float32, -1.0, 1.0)
    x = together(ka, jax.random.normal(kx, shape, jnp.float32), much_x) * bump(kf, D, 4.0)
    dy = together(kb, jax.random.normal(kdy, shape, jnp.float32), much_dy)
    drawn = {"x": x.astype(jnp.bfloat16), "dy": (dy * (SEQUENCES * TOKENS) ** -0.5).astype(jnp.bfloat16)}
    for key, name in zip(kw, NAMES, strict=True):
        w = jax.random.normal(key, SHAPES[name], jnp.float32) * SHAPES[name][1] ** -0.5
        drawn[name] = (w * {"w_gate": 1.0, "w_up": bump(kh, FF, 4.0), "w_down": layers}[name]).astype(jnp.bfloat16)
    return drawn


def matmul(a, w):
    return jnp.dot(a, w, preferred_element_type=jnp.float32).astype(jnp.bfloat16)


def normed(h):
    wide = h.astype(jnp.float32)
    scale = lax.rsqrt(jnp.mean(wide**2, -1, keepdims=True) + 1e-6)
    return (wide * scale).astype(jnp.bfloat16)


def layer(h, w):
    a = normed(h)
    gate = jnp.dot(a, w["w_gate"], preferred_element_type=jnp.float32)
    up = jnp.dot(a, w["w_up"], preferred_element_type=jnp.float32)
    return h + matmul((jax.nn.silu(gate) * up).astype(jnp.bfloat16), w["w_down"])


def stack(weights, h):
    return lax.scan(lambda h, w: (layer(h, w), None), h, weights)[0]


def reference(x, dy, w_gate, w_up, w_down):
    weights = dict(zip(NAMES, (w_gate, w_up, w_down), strict=True))

    def take(so_far, sequence):
        h, by_y = sequence
        _, back = jax.vjp(stack, weights, h)
        by_weights, by_h = back(by_y)
        return jax.tree.map(lambda total, term: total + term.astype(jnp.float32), so_far, by_weights), by_h

    none_yet = {name: jnp.zeros(w.shape, jnp.float32) for name, w in weights.items()}
    by_weights, by_x = lax.scan(take, none_yet, (x, dy))
    return (by_x, *(by_weights[name].astype(jnp.bfloat16) for name in NAMES))
```

```python
import functools

import jax
import jax.numpy as jnp
import numpy as np
from jax import lax
from jax.experimental import pallas as pl
from jax.experimental.pallas import tpu as pltpu
from jax.sharding import PartitionSpec as P

D = 896
FF = 2304
TOK = 2048
C = FF + 1024
BF = jnp.bfloat16
F32 = jnp.float32
MESH = pl.DeviceIdType.MESH
ORDERS = ((0, 1, 2), (1, 2, 0), (2, 0, 1))
ANY = pl.BlockSpec(memory_space=pl.ANY)
VMEM = pl.BlockSpec(memory_space=pltpu.VMEM)


def colours(start, width):
    tiles = width // 128
    out, at = [], start
    for k in range(3):
        n = tiles // 3 + (1 if k < tiles % 3 else 0)
        first = (n + 1) // 2
        out.append(((at, first * 128), (at + first * 128, (n - first) * 128)))
        at += n * 128
    return out


def where():
    me = lax.axis_index("dp")
    return (me // 32, lax.rem(me // 8, 4), lax.rem(me // 2, 4)), lax.rem(me, 2)


def number(xyz, c):
    return ((xyz[0] * 4 + xyz[1]) * 4 + xyz[2]) * 2 + c


def moved(xyz, axis, by):
    out = list(xyz)
    out[axis] = lax.rem(xyz[axis] + by + 4, 4)
    return tuple(out)


def rendezvous(xyz, c):
    barrier = pltpu.get_barrier_semaphore()
    for axis in range(3):
        for by in (1, -1):
            pl.semaphore_signal(barrier, inc=1, device_id={"dp": number(moved(xyz, axis, by), c)}, device_id_type=MESH)
    pl.semaphore_signal(barrier, inc=1, device_id={"dp": number(xyz, 1 - c)}, device_id_type=MESH)
    pl.semaphore_wait(barrier, 7)


def remote(src, dst, send, recv, xyz, c):
    return pltpu.make_async_remote_copy(
        src_ref=src, dst_ref=dst, send_sem=send, recv_sem=recv, device_id={"dp": number(xyz, c)}, device_id_type=MESH
    )


class Gather:
    def __init__(self, cols, shard, g, send, recv, dsend, drecv, lsem):
        self.cols, self.shard, self.g = cols, shard, g
        self.send, self.recv, self.dsend, self.drecv, self.lsem = send, recv, dsend, drecv, lsem
        self.xyz, self.c = where()
        self.pending, self.partner = [], []

    def block(self, k, phase, xyz, half):
        order = ORDERS[k]
        at = [slice(None) if axis in order[:phase] else xyz[axis] for axis in range(3)]
        start, size = self.cols[k][half]
        return self.g.at[at[0], at[1], at[2], self.c, :, pl.ds(start, size)]

    def copy(self, k, phase, owner, half, to, slot, first=False):
        here = self.block(k, phase, owner, half)
        start, size = self.cols[k][half]
        src = self.shard.at[:, pl.ds(start, size)] if first else here
        return remote(src, here, self.send.at[k, phase, slot], self.recv.at[k, phase, slot], to, self.c)

    def local(self):
        return pltpu.make_async_copy(self.shard, self.g.at[self.xyz[0], self.xyz[1], self.xyz[2], self.c], self.lsem)

    def give(self, k, phase, owner, half, slot):
        here = self.block(k, phase, owner, half)
        copy = remote(here, here, self.dsend.at[k, slot], self.drecv.at[k, slot], self.xyz, 1 - self.c)
        copy.start()
        there = self.block_of_partner(k, phase, owner, half)
        self.partner.append((copy, remote(there, there, self.dsend.at[k, slot], self.drecv.at[k, slot], self.xyz, 1 - self.c)))

    def block_of_partner(self, k, phase, owner, half):
        order = ORDERS[k]
        at = [slice(None) if axis in order[:phase] else owner[axis] for axis in range(3)]
        start, size = self.cols[k][half]
        return self.g.at[at[0], at[1], at[2], 1 - self.c, :, pl.ds(start, size)]

    def begin(self, phase):
        if phase == 0:
            self.local().start()
        if phase == 1:
            self.local().wait()
        for k in range(3):
            axis = ORDERS[k][phase]
            right, left = moved(self.xyz, axis, 1), moved(self.xyz, axis, -1)
            for to, half, slot in ((right, 0, 0), (left, 1, 3), (right, 1, 1), (left, 0, 2)):
                copy = self.copy(k, phase, self.xyz, half, to, slot, phase == 0)
                copy.start()
                self.pending.append(copy)
            if phase == 2:
                for half in range(2):
                    self.give(k, 2, self.xyz, half, half)

    def relay(self, phase):
        for k in range(3):
            axis = ORDERS[k][phase]
            right, left = moved(self.xyz, axis, 1), moved(self.xyz, axis, -1)
            for owner, to, half, slot, out in ((left, right, 0, 0, 4), (right, left, 1, 3, 5)):
                self.copy(k, phase, owner, half, to, slot).wait_recv()
                copy = self.copy(k, phase, owner, half, to, out)
                copy.start()
                self.pending.append(copy)
                if phase == 2:
                    self.give(k, 2, owner, half, 2 + half)

    def finish(self, phase):
        for k in range(3):
            axis = ORDERS[k][phase]
            right, left, far = moved(self.xyz, axis, 1), moved(self.xyz, axis, -1), moved(self.xyz, axis, 2)
            for owner, half, slot, give in ((left, 1, 1, 4), (right, 0, 2, 5), (far, 0, 4, 6), (far, 1, 5, 7)):
                self.copy(k, phase, owner, half, owner, slot).wait_recv()
                if phase == 2:
                    self.give(k, 2, owner, half, give)

    def end(self):
        for mine, theirs in self.partner:
            theirs.wait_recv()
            mine.wait_send()
        for copy in self.pending:
            copy.wait_send()

    def steps(self):
        out = []
        for phase in range(3):
            out += [functools.partial(f, phase) for f in (self.begin, self.relay, self.finish)]
        return out + [self.end]


GATHER_SEMS = [
    pltpu.SemaphoreType.DMA((3, 3, 6)),
    pltpu.SemaphoreType.DMA((3, 3, 6)),
    pltpu.SemaphoreType.DMA((3, 8)),
    pltpu.SemaphoreType.DMA((3, 8)),
    pltpu.SemaphoreType.DMA,
]


def gather_kernel(cols, shard, g, *sems):
    gather = Gather(cols, shard, g, *sems)
    rendezvous(gather.xyz, gather.c)
    for step in gather.steps():
        step()


def gather_call(shard, collective_id):
    width = shard.shape[1]
    return pl.pallas_call(
        functools.partial(gather_kernel, colours(0, width)),
        out_shape=jax.ShapeDtypeStruct((4, 4, 4, 2, 16, width), BF),
        in_specs=[VMEM],
        out_specs=ANY,
        scratch_shapes=GATHER_SEMS,
        compiler_params=pltpu.CompilerParams(collective_id=collective_id, has_side_effects=True),
        name="gather",
    )(shard)


class Scatter:
    def __init__(self, cols, d, out, own, pair, keep, one, left2, right2, next_, send, recv, dsend, drecv, lsem):
        self.cols, self.d, self.out, self.own, self.pair = cols, d, out, own, pair
        self.keep, self.one, self.l2, self.r2, self.next = keep, one, left2, right2, next_
        self.send, self.recv, self.dsend, self.drecv, self.lsem = send, recv, dsend, drecv, lsem
        self.xyz, self.c = where()
        self.pending = []

    def local(self, k):
        (start, n0), (_, n1) = self.cols[k]
        at = pl.ds(start, n0 + n1)
        return pltpu.make_async_copy(self.d.at[:, :, :, self.c, :, at], self.own.at[:, :, :, :, at], self.lsem.at[k])

    def swap(self, k):
        (start, n0), (_, n1) = self.cols[k]
        at = pl.ds(start, n0 + n1)
        return remote(
            self.d.at[:, :, :, 1 - self.c, :, at], self.pair.at[:, :, :, :, at], self.dsend.at[k], self.drecv.at[k], self.xyz, 1 - self.c
        )

    def begin_swap(self):
        for k in range(3):
            self.local(k).start()
            self.swap(k).start()

    def cut(self, k, half):
        start, size = self.cols[k][half]
        return pl.ds(start, size)

    def both(self, k):
        (start, n0), (_, n1) = self.cols[k]
        return pl.ds(start, n0 + n1)

    def add_swap(self, k):
        self.local(k).wait()
        self.swap(k).wait_recv()
        at, axis = self.both(k), ORDERS[k][0]

        def body(i, _):
            xyz = (i // 16, lax.rem(i // 4, 4), lax.rem(i, 4))
            here = (*xyz, slice(None), at)
            total = self.own[here].astype(F32) + self.pair[here].astype(F32)
            self.own[here] = total.astype(BF)
            rest = [xyz[a] for a in range(3) if a != axis]

            @pl.when(xyz[axis] == self.xyz[axis])
            def _():
                self.keep[0][(*rest, slice(None), at)] = total

            return 0

        lax.fori_loop(0, 64, body, 0)

    def source(self, k, phase, where_):
        order = ORDERS[k]
        if phase == 0:
            return [where_ if a == order[0] else slice(None) for a in range(3)]
        if phase == 1:
            rest = [a for a in range(3) if a != order[0]]
            return [where_ if a == order[1] else slice(None) for a in rest]
        return [where_]

    def buf(self, phase):
        return self.own if phase == 0 else self.next[phase - 1]

    def copy(self, k, phase, half, slot, to, to_at, dst):
        src = self.buf(phase).at[(*self.source(k, phase, to_at), slice(None), self.cut(k, half))]
        lead = [slice(None)] * (2 - phase)
        there = dst[phase].at[(*lead, slice(None), self.cut(k, half))]
        return remote(src, there, self.send.at[k, phase, slot], self.recv.at[k, phase, slot], to, self.c)

    def sides(self, k, phase):
        axis = ORDERS[k][phase]
        right, left = moved(self.xyz, axis, 1), moved(self.xyz, axis, -1)
        return right, left, right[axis], left[axis], lax.rem(self.xyz[axis] + 2, 4)

    def first(self, k, phase):
        right, left, ri, li, far = self.sides(k, phase)
        for copy in (
            self.copy(k, phase, 0, 0, right, far, self.one),
            self.copy(k, phase, 1, 1, left, far, self.one),
            self.copy(k, phase, 1, 2, right, ri, self.l2),
            self.copy(k, phase, 0, 3, left, li, self.r2),
        ):
            copy.start()
            self.pending.append(copy)

    def shards(self, phase):
        return (16, 4, 1)[phase]

    def lead(self, phase, i):
        return ((i // 4, lax.rem(i, 4)), (i,), ())[phase]

    def second(self, k, phase):
        right, left, ri, li, far = self.sides(k, phase)
        for half, slot, to, to_at, dst, out in ((0, 0, right, ri, self.l2, 4), (1, 1, left, li, self.r2, 5)):
            self.copy(k, phase, half, slot, to, far, self.one).wait_recv()
            at, buf = self.cut(k, half), self.buf(phase)
            where_ = self.source(k, phase, to_at)

            def body(i, _):
                lead = self.lead(phase, i)
                it = iter(lead)
                idx = tuple(next(it) if isinstance(w, slice) else w for w in where_)
                here = (*idx, slice(None), at)
                got = self.one[phase][(*lead, slice(None), at)]
                buf[here] = (buf[here].astype(F32) + got.astype(F32)).astype(BF)
                return 0

            lax.fori_loop(0, self.shards(phase), body, 0)
            copy = self.copy(k, phase, half, out, to, to_at, dst)
            copy.start()
            self.pending.append(copy)

    def third(self, k, phase):
        right, left, ri, li, far = self.sides(k, phase)
        for half, slot, dst in ((1, 2, self.l2), (0, 3, self.r2), (0, 4, self.l2), (1, 5, self.r2)):
            self.copy(k, phase, half, slot, right, ri, dst).wait_recv()
        at, order = self.both(k), ORDERS[k]

        def body(i, _):
            lead = self.lead(phase, i)
            here = (*lead, slice(None), at)
            total = self.keep[phase][here] + self.l2[phase][here].astype(F32) + self.r2[phase][here].astype(F32)
            if phase == 2:
                self.out[:, at] = total.astype(BF)
                return 0
            self.next[phase][here] = total.astype(BF)
            if phase == 0:
                rest = [a for a in range(3) if a != order[0]]
                mine = [n for n, a in zip(lead, rest) if a == order[1]][0]
                other = tuple(n for n, a in zip(lead, rest) if a != order[1])
            else:
                mine, other = lead[0], ()

            @pl.when(mine == self.xyz[order[phase + 1]])
            def _():
                self.keep[phase + 1][(*other, slice(None), at)] = total

            return 0

        lax.fori_loop(0, self.shards(phase), body, 0)

    def end(self):
        for k in range(3):
            self.swap(k).wait_send()
        for copy in self.pending:
            copy.wait_send()

    def steps(self):
        out = [self.begin_swap]
        for k in range(3):
            out += [functools.partial(self.add_swap, k), functools.partial(self.first, k, 0)]
        for phase in range(3):
            out += [functools.partial(self.second, k, phase) for k in range(3)]
            for k in range(3):
                out.append(functools.partial(self.third, k, phase))
                if phase < 2:
                    out.append(functools.partial(self.first, k, phase + 1))
        return out + [self.end]


def scatter_scratch(width):
    w = (16, width)
    leads = ((4, 4), (4,), ())
    return [
        pltpu.VMEM((4, 4, 4, *w), BF),
        pltpu.VMEM((4, 4, 4, *w), BF),
        *[pltpu.VMEM((*lead, *w), F32) for lead in leads],
        *[pltpu.VMEM((*lead, *w), BF) for _ in range(3) for lead in leads],
        *[pltpu.VMEM((*lead, *w), BF) for lead in leads[:2]],
        pltpu.SemaphoreType.DMA((3, 3, 6)),
        pltpu.SemaphoreType.DMA((3, 3, 6)),
        pltpu.SemaphoreType.DMA((3,)),
        pltpu.SemaphoreType.DMA((3,)),
        pltpu.SemaphoreType.DMA((3,)),
    ]


def make_scatter(cols, d, out, scratch):
    own, pair = scratch[:2]
    keep, one, l2, r2, next_ = scratch[2:5], scratch[5:8], scratch[8:11], scratch[11:14], scratch[14:16]
    return Scatter(cols, d, out, own, pair, keep, one, l2, r2, next_, *scratch[16:])


def scatter_kernel(cols, d, out, *scratch):
    scatter = make_scatter(cols, d, out, scratch)
    rendezvous(scatter.xyz, scatter.c)
    for step in scatter.steps():
        step()


def scatter_call(d, collective_id):
    width = d.shape[-1]
    return pl.pallas_call(
        functools.partial(scatter_kernel, colours(0, width)),
        out_shape=jax.ShapeDtypeStruct((16, width), BF),
        in_specs=[ANY],
        out_specs=VMEM,
        scratch_shapes=scatter_scratch(width),
        compiler_params=pltpu.CompilerParams(collective_id=collective_id, has_side_effects=True, vmem_limit_bytes=60 * 2**20),
        name="scatter",
    )(d)


def picks():
    gu = np.zeros((224, 256), np.float32)
    main = np.zeros((288, 256), np.float32)
    extra = np.zeros((7, 288, 256), np.float32)
    for d in range(16):
        for j in range(7):
            gu[7 * d + j, 16 * d + j] = 1
            gu[112 + 7 * d + j, 16 * d + 8 + j] = 1
        for r in range(16):
            main[18 * d + r, 16 * d + r] = 1
        for e in range(2):
            for t in range(7):
                extra[t, 18 * d + 16 + e, 16 * d + 7 * e + t] = 1
    return tuple(jnp.asarray(t, BF) for t in (gu, main, extra))


def one_hot(spec, *args):
    return jnp.einsum(spec, *args, preferred_element_type=F32)


def pack_shard(gate, up, down):
    row = ((0, 1), (0, 0))
    gu = jnp.concatenate([jnp.pad(gate, row), jnp.pad(up, row)], 0)
    rest = jnp.pad(down[16:].reshape(14, 128), ((0, 2), (0, 0)))
    return jnp.concatenate([gu, down[:16], rest], 1)


def unpack_shard(p):
    gate, up = p[:7, :FF], p[8:15, :FF]
    down = jnp.concatenate([p[:, FF : FF + D], p[:14, FF + D :].reshape(2, D)], 0)
    return gate, up, down


def unpack_gu(g):
    gu = picks()[0]
    w = one_hot("rk,gkn->grn", gu, g.reshape(8, 256, FF)).astype(BF)
    return w[:, :112].reshape(D, FF), w[:, 112:].reshape(D, FF)


def unpack_down(g):
    _, main, extra = picks()
    g = g.reshape(8, 256, 1024)
    w = one_hot("rk,gkn->grn", main, g[..., :D]).reshape(8, 288, 7, 128) + one_hot("trk,gkn->grtn", extra, g[..., D:])
    return w.astype(BF).reshape(FF, D)


def pack_gu(gate, up):
    gu = picks()[0]
    w = jnp.concatenate([gate.reshape(8, 112, FF), up.reshape(8, 112, FF)], 1)
    return one_hot("rk,grn->gkn", gu, w).astype(BF).reshape(4, 4, 4, 2, 16, FF)


def pack_down(down):
    _, main, extra = picks()
    w = down.reshape(8, 288, D)
    a = one_hot("rk,grn->gkn", main, w)
    b = one_hot("trk,grtn->gkn", extra, w.reshape(8, 288, 7, 128))
    return jnp.concatenate([a, b], -1).astype(BF).reshape(4, 4, 4, 2, 16, 1024)


def matmul(a, w):
    return jnp.dot(a, w, preferred_element_type=F32).astype(BF)


def normed(h):
    wide = h.astype(F32)
    scale = lax.rsqrt(jnp.mean(wide**2, -1, keepdims=True) + 1e-6)
    return (wide * scale).astype(BF)


def layer(h, w):
    a = normed(h)
    gate = jnp.dot(a, w[0], preferred_element_type=F32)
    up = jnp.dot(a, w[1], preferred_element_type=F32)
    return h + matmul((jax.nn.silu(gate) * up).astype(BF), w[2])


def stack(weights, h):
    for w in weights:
        h = layer(h, w)
    return h


def solution(mesh):
    def step(x, dy, gate, up, down):
        shard = jnp.concatenate([pack_shard(gate[n], up[n], down[n]) for n in range(2)], 1)
        g = gather_call(shard, 0)
        weights = []
        for n in range(2):
            part = g[..., n * C : (n + 1) * C]
            weights.append((*unpack_gu(part[..., :FF]), unpack_down(part[..., FF:])))
        _, back = jax.vjp(stack, weights, x[0])
        by_weights, by_x = back(dy[0])
        outs = []
        for n in (1, 0):
            dg, du, dd = by_weights[n]
            d = jnp.concatenate([pack_gu(dg, du), pack_down(dd)], -1)
            outs.append(unpack_shard(scatter_call(d, 1)))
        outs = outs[::-1]
        return (by_x[None], *(jnp.stack([o[i] for o in outs]) for i in range(3)))

    rows = P(None, "dp", None)
    return jax.shard_map(
        step, mesh=mesh, in_specs=(P("dp"), P("dp"), rows, rows, rows), out_specs=(P("dp"), rows, rows, rows), check_vma=False
    )
```

```python
import functools

import jax
import jax.numpy as jnp
import numpy as np
from jax import lax
from jax.experimental import pallas as pl
from jax.experimental.pallas import tpu as pltpu
from jax.sharding import PartitionSpec as P

D = 896
FF = 2304
TOK = 2048
C = FF + 1024
BF = jnp.bfloat16
F32 = jnp.float32
MESH = pl.DeviceIdType.MESH
ORDERS = ((0, 1, 2), (1, 2, 0), (2, 0, 1))
ANY = pl.BlockSpec(memory_space=pl.ANY)
VMEM = pl.BlockSpec(memory_space=pltpu.VMEM)


def colours(start, width):
    tiles = width // 128
    out, at = [], start
    for k in range(3):
        n = tiles // 3 + (1 if k < tiles % 3 else 0)
        first = (n + 1) // 2
        out.append(((at, first * 128), (at + first * 128, (n - first) * 128)))
        at += n * 128
    return out


def where():
    me = lax.axis_index("dp")
    return (me // 32, lax.rem(me // 8, 4), lax.rem(me // 2, 4)), lax.rem(me, 2)


def number(xyz, c):
    return ((xyz[0] * 4 + xyz[1]) * 4 + xyz[2]) * 2 + c


def moved(xyz, axis, by):
    out = list(xyz)
    out[axis] = lax.rem(xyz[axis] + by + 4, 4)
    return tuple(out)


def rendezvous(xyz, c):
    barrier = pltpu.get_barrier_semaphore()
    for axis in range(3):
        for by in (1, -1):
            pl.semaphore_signal(barrier, inc=1, device_id={"dp": number(moved(xyz, axis, by), c)}, device_id_type=MESH)
    pl.semaphore_signal(barrier, inc=1, device_id={"dp": number(xyz, 1 - c)}, device_id_type=MESH)
    pl.semaphore_wait(barrier, 7)


def remote(src, dst, send, recv, xyz, c):
    return pltpu.make_async_remote_copy(
        src_ref=src, dst_ref=dst, send_sem=send, recv_sem=recv, device_id={"dp": number(xyz, c)}, device_id_type=MESH
    )


class Gather:
    def __init__(self, cols, shard, g, send, recv, dsend, drecv, lsem):
        self.cols, self.shard, self.g = cols, shard, g
        self.send, self.recv, self.dsend, self.drecv, self.lsem = send, recv, dsend, drecv, lsem
        self.xyz, self.c = where()
        self.pending, self.partner = [], []

    def at(self, k, phase, by):
        return moved(self.xyz, ORDERS[k][phase], by)

    def block(self, k, phase, by, half, c):
        order, xyz = ORDERS[k], self.at(k, phase, by)
        at = [slice(None) if axis in order[:phase] else xyz[axis] for axis in range(3)]
        start, size = self.cols[k][half]
        return self.g.at[at[0], at[1], at[2], c, :, pl.ds(start, size)]

    def copy(self, k, phase, owner, half, to, slot):
        here = self.block(k, phase, owner, half, self.c)
        start, size = self.cols[k][half]
        src = self.shard.at[:, pl.ds(start, size)] if phase == 0 and owner == 0 else here
        return remote(src, here, self.send.at[k, phase, slot], self.recv.at[k, phase, slot], self.at(k, phase, to), self.c)

    def local(self):
        return pltpu.make_async_copy(self.shard, self.g.at[self.xyz[0], self.xyz[1], self.xyz[2], self.c], self.lsem)

    def over(self, k, phase, owner, half, slot, c):
        here = self.block(k, phase, owner, half, c)
        return remote(here, here, self.dsend.at[k, slot], self.drecv.at[k, slot], self.xyz, 1 - self.c)

    def go(self, *what):
        self.copy(*what).start()
        self.pending.append(what)

    def give(self, *what):
        self.over(*what, self.c).start()
        self.partner.append(what)

    def begin(self, phase):
        if phase == 0:
            self.local().start()
        if phase == 1:
            self.local().wait()
        for k in range(3):
            for to, half, slot in ((1, 0, 0), (-1, 1, 3), (1, 1, 1), (-1, 0, 2)):
                self.go(k, phase, 0, half, to, slot)
            if phase == 2:
                for half in range(2):
                    self.give(k, 2, 0, half, half)

    def relay(self, phase):
        for k in range(3):
            for owner, to, half, slot, out in ((-1, 1, 0, 0, 4), (1, -1, 1, 3, 5)):
                self.copy(k, phase, owner, half, to, slot).wait_recv()
                self.go(k, phase, owner, half, to, out)
                if phase == 2:
                    self.give(k, 2, owner, half, 2 + half)

    def finish(self, phase):
        for k in range(3):
            for owner, half, slot, give in ((-1, 1, 1, 4), (1, 0, 2, 5), (2, 0, 4, 6), (2, 1, 5, 7)):
                self.copy(k, phase, owner, half, 1, slot).wait_recv()
                if phase == 2:
                    self.give(k, 2, owner, half, give)

    def end(self):
        for what in self.partner:
            self.over(*what, 1 - self.c).wait_recv()
            self.over(*what, self.c).wait_send()
        for what in self.pending:
            self.copy(*what).wait_send()

    def steps(self):
        out = [functools.partial(self.begin, 0), functools.partial(self.relay, 0)]
        for phase in (1, 2):
            out += [functools.partial(self.turn, phase), functools.partial(self.relay, phase)]
        return out + [functools.partial(self.finish, 2), self.end]

    def turn(self, phase):
        self.finish(phase - 1)
        self.begin(phase)


GATHER_SEMS = [
    pltpu.SemaphoreType.DMA((3, 3, 6)),
    pltpu.SemaphoreType.DMA((3, 3, 6)),
    pltpu.SemaphoreType.DMA((3, 8)),
    pltpu.SemaphoreType.DMA((3, 8)),
    pltpu.SemaphoreType.DMA,
]


def gather_kernel(cols, shard, g, *sems):
    gather = Gather(cols, shard, g, *sems)
    rendezvous(gather.xyz, gather.c)
    for step in gather.steps():
        step()


def gather_call(shard, collective_id):
    width = shard.shape[1]
    return pl.pallas_call(
        functools.partial(gather_kernel, colours(0, width)),
        out_shape=jax.ShapeDtypeStruct((4, 4, 4, 2, 16, width), BF),
        in_specs=[VMEM],
        out_specs=ANY,
        scratch_shapes=GATHER_SEMS,
        compiler_params=pltpu.CompilerParams(collective_id=collective_id, has_side_effects=True),
        name="gather",
    )(shard)


class Scatter:
    def __init__(self, cols, d, out, own, pair, keep, one, left2, right2, next_, send, recv, dsend, drecv, lsem):
        self.cols, self.d, self.out, self.own, self.pair = cols, d, out, own, pair
        self.keep, self.one, self.l2, self.r2, self.next = keep, one, left2, right2, next_
        self.send, self.recv, self.dsend, self.drecv, self.lsem = send, recv, dsend, drecv, lsem
        self.xyz, self.c = where()
        self.pending = []

    def local(self, k):
        (start, n0), (_, n1) = self.cols[k]
        at = pl.ds(start, n0 + n1)
        return pltpu.make_async_copy(self.d.at[:, :, :, self.c, :, at], self.own.at[:, :, :, :, at], self.lsem.at[k])

    def swap(self, k):
        (start, n0), (_, n1) = self.cols[k]
        at = pl.ds(start, n0 + n1)
        return remote(
            self.d.at[:, :, :, 1 - self.c, :, at], self.pair.at[:, :, :, :, at], self.dsend.at[k], self.drecv.at[k], self.xyz, 1 - self.c
        )

    def begin_swap(self):
        for k in range(3):
            self.local(k).start()
            self.swap(k).start()

    def cut(self, k, half):
        start, size = self.cols[k][half]
        return pl.ds(start, size)

    def both(self, k):
        (start, n0), (_, n1) = self.cols[k]
        return pl.ds(start, n0 + n1)

    def add_swap(self, k):
        self.local(k).wait()
        self.swap(k).wait_recv()
        at, axis = self.both(k), ORDERS[k][0]

        def body(i, _):
            xyz = (i // 16, lax.rem(i // 4, 4), lax.rem(i, 4))
            here = (*xyz, slice(None), at)
            total = self.own[here].astype(F32) + self.pair[here].astype(F32)
            self.own[here] = total.astype(BF)
            rest = [xyz[a] for a in range(3) if a != axis]

            @pl.when(xyz[axis] == self.xyz[axis])
            def _():
                self.keep[0][(*rest, slice(None), at)] = total

            return 0

        lax.fori_loop(0, 64, body, 0)

    def source(self, k, phase, where_):
        order = ORDERS[k]
        if phase == 0:
            return [where_ if a == order[0] else slice(None) for a in range(3)]
        if phase == 1:
            rest = [a for a in range(3) if a != order[0]]
            return [where_ if a == order[1] else slice(None) for a in rest]
        return [where_]

    def buf(self, phase):
        return self.own if phase == 0 else self.next[phase - 1]

    def copy(self, k, phase, half, slot, to, to_at, dst):
        axis = ORDERS[k][phase]
        at, to = moved(self.xyz, axis, to_at)[axis], moved(self.xyz, axis, to)
        src = self.buf(phase).at[(*self.source(k, phase, at), slice(None), self.cut(k, half))]
        lead = [slice(None)] * (2 - phase)
        there = dst[phase].at[(*lead, slice(None), self.cut(k, half))]
        return remote(src, there, self.send.at[k, phase, slot], self.recv.at[k, phase, slot], to, self.c)

    def go(self, *what):
        self.copy(*what).start()
        self.pending.append(what)

    def first(self, k, phase):
        self.go(k, phase, 0, 0, 1, 2, self.one)
        self.go(k, phase, 1, 1, -1, 2, self.one)
        self.go(k, phase, 1, 2, 1, 1, self.l2)
        self.go(k, phase, 0, 3, -1, -1, self.r2)

    def shards(self, phase):
        return (16, 4, 1)[phase]

    def lead(self, phase, i):
        return ((i // 4, lax.rem(i, 4)), (i,), ())[phase]

    def second(self, k, phase):
        axis = ORDERS[k][phase]
        for half, slot, to, dst, out in ((0, 0, 1, self.l2, 4), (1, 1, -1, self.r2, 5)):
            self.copy(k, phase, half, slot, to, 2, self.one).wait_recv()
            at, buf = self.cut(k, half), self.buf(phase)
            where_ = self.source(k, phase, moved(self.xyz, axis, to)[axis])

            def body(i, _):
                lead = self.lead(phase, i)
                it = iter(lead)
                idx = tuple(next(it) if isinstance(w, slice) else w for w in where_)
                here = (*idx, slice(None), at)
                got = self.one[phase][(*lead, slice(None), at)]
                buf[here] = (buf[here].astype(F32) + got.astype(F32)).astype(BF)
                return 0

            lax.fori_loop(0, self.shards(phase), body, 0)
            self.go(k, phase, half, out, to, to, dst)

    def third(self, k, phase):
        for half, slot, dst in ((1, 2, self.l2), (0, 3, self.r2), (0, 4, self.l2), (1, 5, self.r2)):
            self.copy(k, phase, half, slot, 1, 1, dst).wait_recv()
        at, order = self.both(k), ORDERS[k]

        def body(i, _):
            lead = self.lead(phase, i)
            here = (*lead, slice(None), at)
            total = self.keep[phase][here] + self.l2[phase][here].astype(F32) + self.r2[phase][here].astype(F32)
            if phase == 2:
                self.out[:, at] = total.astype(BF)
                return 0
            self.next[phase][here] = total.astype(BF)
            if phase == 0:
                rest = [a for a in range(3) if a != order[0]]
                mine = [n for n, a in zip(lead, rest) if a == order[1]][0]
                other = tuple(n for n, a in zip(lead, rest) if a != order[1])
            else:
                mine, other = lead[0], ()

            @pl.when(mine == self.xyz[order[phase + 1]])
            def _():
                self.keep[phase + 1][(*other, slice(None), at)] = total

            return 0

        lax.fori_loop(0, self.shards(phase), body, 0)

    def end(self):
        for k in range(3):
            self.swap(k).wait_send()
        for what in self.pending:
            self.copy(*what).wait_send()

    def opened(self, k):
        self.add_swap(k)
        self.first(k, 0)

    def seconds(self, phase):
        for k in range(3):
            self.second(k, phase)

    def thirds(self, phase):
        for k in range(3):
            self.third(k, phase)
            if phase < 2:
                self.first(k, phase + 1)

    def steps(self):
        out = [self.begin_swap, *[functools.partial(self.opened, k) for k in range(3)]]
        for phase in range(3):
            out += [functools.partial(self.seconds, phase), functools.partial(self.thirds, phase)]
        return out + [self.end]


def scatter_scratch(width):
    w = (16, width)
    leads = ((4, 4), (4,), ())
    return [
        pltpu.VMEM((4, 4, 4, *w), BF),
        pltpu.VMEM((4, 4, 4, *w), BF),
        *[pltpu.VMEM((*lead, *w), F32) for lead in leads],
        *[pltpu.VMEM((*lead, *w), BF) for _ in range(3) for lead in leads],
        *[pltpu.VMEM((*lead, *w), BF) for lead in leads[:2]],
        pltpu.SemaphoreType.DMA((3, 3, 6)),
        pltpu.SemaphoreType.DMA((3, 3, 6)),
        pltpu.SemaphoreType.DMA((3,)),
        pltpu.SemaphoreType.DMA((3,)),
        pltpu.SemaphoreType.DMA((3,)),
    ]


def make_scatter(cols, d, out, scratch):
    own, pair = scratch[:2]
    keep, one, l2, r2, next_ = scratch[2:5], scratch[5:8], scratch[8:11], scratch[11:14], scratch[14:16]
    return Scatter(cols, d, out, own, pair, keep, one, l2, r2, next_, *scratch[16:])


def scatter_kernel(cols, d, out, *scratch):
    scatter = make_scatter(cols, d, out, scratch)
    rendezvous(scatter.xyz, scatter.c)
    for step in scatter.steps():
        step()


def scatter_call(d, collective_id):
    width = d.shape[-1]
    return pl.pallas_call(
        functools.partial(scatter_kernel, colours(0, width)),
        out_shape=jax.ShapeDtypeStruct((16, width), BF),
        in_specs=[ANY],
        out_specs=VMEM,
        scratch_shapes=scatter_scratch(width),
        compiler_params=pltpu.CompilerParams(collective_id=collective_id, has_side_effects=True, vmem_limit_bytes=60 * 2**20),
        name="scatter",
    )(d)


def picks():
    gu = np.zeros((224, 256), np.float32)
    main = np.zeros((288, 256), np.float32)
    extra = np.zeros((7, 288, 256), np.float32)
    for d in range(16):
        for j in range(7):
            gu[7 * d + j, 16 * d + j] = 1
            gu[112 + 7 * d + j, 16 * d + 8 + j] = 1
        for r in range(16):
            main[18 * d + r, 16 * d + r] = 1
        for e in range(2):
            for t in range(7):
                extra[t, 18 * d + 16 + e, 16 * d + 7 * e + t] = 1
    return tuple(jnp.asarray(t, BF) for t in (gu, main, extra))


def one_hot(spec, *args):
    return jnp.einsum(spec, *args, preferred_element_type=F32)


def pack_shard(gate, up, down):
    row = ((0, 1), (0, 0))
    gu = jnp.concatenate([jnp.pad(gate, row), jnp.pad(up, row)], 0)
    rest = jnp.pad(down[16:].reshape(14, 128), ((0, 2), (0, 0)))
    return jnp.concatenate([gu, down[:16], rest], 1)


def unpack_shard(p):
    gate, up = p[:7, :FF], p[8:15, :FF]
    down = jnp.concatenate([p[:, FF : FF + D], p[:14, FF + D :].reshape(2, D)], 0)
    return gate, up, down


def unpack_kernel(g, gu, main, extra, wg, wu, wd):
    both = one_hot("rk,kn->rn", gu[...], g[0, :, :FF]).astype(BF)
    wg[...] = both[:112]
    wu[...] = both[112:]
    first = one_hot("rk,kn->rn", main[...], g[0, :, FF : FF + D])
    for t in range(7):
        at = slice(128 * t, 128 * t + 128)
        wd[:, at] = (first[:, at] + one_hot("rk,kn->rn", extra[t], g[0, :, FF + D :])).astype(BF)


def whole(shape):
    return pl.BlockSpec(shape, lambda i: (0,) * len(shape), pipeline_mode=pl.Buffered(1))


def rows(n, width):
    return pl.BlockSpec((n, width), lambda i: (i, 0))


def like(n, width, dtype=BF):
    return jax.ShapeDtypeStruct((n, width), dtype)


def params(**more):
    return pltpu.CompilerParams(dimension_semantics=("arbitrary",), vmem_limit_bytes=62 * 2**20, **more)


PICKS = [whole((224, 256)), whole((288, 256)), whole((7, 288, 256))]


def unpack(g):
    return pl.pallas_call(
        unpack_kernel,
        grid=(8,),
        in_specs=[pl.BlockSpec((1, 256, C), lambda i: (i, 0, 0)), *PICKS],
        out_specs=[rows(112, FF), rows(112, FF), rows(288, D)],
        out_shape=[like(D, FF), like(D, FF), like(FF, D)],
        compiler_params=params(),
        name="unpack",
    )(g.reshape(8, 256, C), *picks())


def pack_kernel(dg, du, dd, gu, main, extra, out):
    both = jnp.concatenate([dg[...], du[...]], 0)
    out[0, :, :FF] = one_hot("rk,rn->kn", gu[...], both).astype(BF)
    out[0, :, FF : FF + D] = one_hot("rk,rn->kn", main[...], dd[...]).astype(BF)
    last = jnp.zeros((256, 128), F32)
    for t in range(7):
        last += one_hot("rk,rn->kn", extra[t], dd[:, 128 * t : 128 * t + 128])
    out[0, :, FF + D :] = last.astype(BF)


def pack(dg, du, dd):
    out = pl.pallas_call(
        pack_kernel,
        grid=(8,),
        in_specs=[rows(112, FF), rows(112, FF), rows(288, D), *PICKS],
        out_specs=pl.BlockSpec((1, 256, C), lambda i: (i, 0, 0)),
        out_shape=jax.ShapeDtypeStruct((8, 256, C), BF),
        compiler_params=params(),
        name="pack",
    )(dg, du, dd, *picks())
    return out.reshape(4, 4, 4, 2, 16, C)


CHUNK = 768
CHUNKS = tuple(slice(at, at + CHUNK) for at in range(0, FF, CHUNK))


def mm(a, w):
    return lax.dot_general(a, w, (((1,), (0,)), ((), ())), preferred_element_type=F32)


def mmt(a, w):
    return lax.dot_general(a, w, (((1,), (1,)), ((), ())), preferred_element_type=F32)


def norm(h):
    wide = h.astype(F32)
    scale = lax.rsqrt(jnp.mean(wide * wide, -1, keepdims=True) + 1e-6)
    return wide, scale


def norm_back(wide, scale, da, dh):
    da = da.astype(BF).astype(F32)
    inner = jnp.mean(da * wide, -1, keepdims=True)
    by_h = (da * scale - wide * (scale * scale * scale * inner)).astype(BF)
    return (dh.astype(F32) + by_h.astype(F32)).astype(BF)


def gate_back(g, u, ds):
    sig = 1.0 / (1.0 + jnp.exp(-g))
    soft = g * sig
    du = (ds * soft).astype(BF)
    dg = (ds * u * (sig * (1.0 + g - soft))).astype(BF)
    return soft, dg, du


def at_step(number, step):
    @pl.when(pl.program_id(0) == number)
    def _():
        step()


def forward_kernel(x, wg, wu, wd, shard, h, a_out, g_out, u_out, s_out, gathered, *sems):
    gather = Gather(colours(0, C), shard, gathered, *sems)
    steps = gather.steps()

    def start():
        rendezvous(gather.xyz, gather.c)
        steps[0]()

    at_step(0, start)
    for n, step in enumerate(steps[1:-1]):
        at_step(n + 1, step)
    wide, scale = norm(x[...])
    a = (wide * scale).astype(BF)
    a_out[...] = a
    for at in CHUNKS:
        g, u = mm(a, wg[:, at]), mm(a, wu[:, at])
        g_out[:, at] = g
        u_out[:, at] = u
        s_out[:, at] = (g * (1.0 / (1.0 + jnp.exp(-g))) * u).astype(BF)
    h[...] = (x[...].astype(F32) + mm(s_out[...], wd[...]).astype(BF).astype(F32)).astype(BF)
    at_step(7, steps[-1])


def forward(x, weights, shard):
    n = TOK // 8
    return pl.pallas_call(
        forward_kernel,
        grid=(8,),
        in_specs=[rows(n, D), whole((D, FF)), whole((D, FF)), whole((FF, D)), whole((16, C))],
        out_specs=[rows(n, D), rows(n, D), rows(n, FF), rows(n, FF), rows(n, FF), ANY],
        out_shape=[
            like(TOK, D), like(TOK, D), like(TOK, FF, F32), like(TOK, FF, F32), like(TOK, FF),
            jax.ShapeDtypeStruct((4, 4, 4, 2, 16, C), BF),
        ],
        scratch_shapes=GATHER_SEMS,
        compiler_params=params(collective_id=2, has_side_effects=True),
        name="forward",
    )(x, *weights, shard)


def middle_kernel(h, dy, wg, wu, wd, a_out, s_out, dg_out, du_out, dh):
    wide, scale = norm(h[...])
    a = (wide * scale).astype(BF)
    a_out[...] = a
    da = None
    for at in CHUNKS:
        g, u = mm(a, wg[:, at]), mm(a, wu[:, at])
        ds = mmt(dy[...], wd[at, :]).astype(BF).astype(F32)
        soft, dg, du = gate_back(g, u, ds)
        s_out[:, at] = (soft * u).astype(BF)
        dg_out[:, at] = dg
        du_out[:, at] = du
    da = mmt(dg_out[...], wg[...]) + mmt(du_out[...], wu[...])
    dh[...] = norm_back(wide, scale, da, dy[...])


def middle(h, dy, weights):
    n = TOK // 4
    return pl.pallas_call(
        middle_kernel,
        grid=(4,),
        in_specs=[rows(n, D), rows(n, D), whole((D, FF)), whole((D, FF)), whole((FF, D))],
        out_specs=[rows(n, D), rows(n, FF), rows(n, FF), rows(n, FF), rows(n, D)],
        out_shape=[like(TOK, D), like(TOK, FF), like(TOK, FF), like(TOK, FF), like(TOK, D)],
        compiler_params=params(),
        name="middle",
    )(h, dy, *weights)


def backward_kernel(x, dh, g_in, u_in, wg, wu, wd, d, dg_out, du_out, dx, summed, *scratch):
    scatter = make_scatter(colours(0, C), d, summed, scratch)
    steps = scatter.steps()

    def start():
        rendezvous(scatter.xyz, scatter.c)
        steps[0]()

    at_step(0, start)
    when = {3: (1, 2), 4: (3,), 6: (4,)}
    for number, group in when.items():
        for n in group:
            at_step(number, steps[n])
    for at in CHUNKS:
        ds = mmt(dh[...], wd[at, :]).astype(BF).astype(F32)
        _, dg, du = gate_back(g_in[:, at], u_in[:, at], ds)
        dg_out[:, at] = dg
        du_out[:, at] = du
    wide, scale = norm(x[...])
    da = mmt(dg_out[...], wg[...]) + mmt(du_out[...], wu[...])
    dx[...] = norm_back(wide, scale, da, dh[...])
    for step in steps[5:]:
        at_step(7, step)


def backward(x, dh, g, u, weights, d):
    n = TOK // 8
    return pl.pallas_call(
        backward_kernel,
        grid=(8,),
        in_specs=[rows(n, D), rows(n, D), rows(n, FF), rows(n, FF), whole((D, FF)), whole((D, FF)), whole((FF, D)), ANY],
        out_specs=[rows(n, FF), rows(n, FF), rows(n, D), pl.BlockSpec((16, C), lambda i: (0, 0))],
        out_shape=[like(TOK, FF), like(TOK, FF), like(TOK, D), like(16, C)],
        scratch_shapes=scatter_scratch(C),
        compiler_params=params(collective_id=3, has_side_effects=True),
        name="backward",
    )(x, dh, g, u, *weights, d)


def turned(a, b):
    return lax.dot_general(a, b, (((0,), (0,)), ((), ())), preferred_element_type=F32).astype(BF)


def solution(mesh):
    def step(x, dy, gate, up, down):
        x, dy = x[0], dy[0]
        shards = [pack_shard(gate[n], up[n], down[n]) for n in range(2)]
        w0 = unpack(gather_call(shards[0], 0))
        h, a0, g0, u0, s0, g1 = forward(x, w0, shards[1])
        a1, s1, dg1, du1, dh = middle(h, dy, unpack(g1))
        d1 = pack(turned(a1, dg1), turned(a1, du1), turned(s1, dy))
        dg0, du0, dx, sum1 = backward(x, dh, g0, u0, w0, d1)
        d0 = pack(turned(a0, dg0), turned(a0, du0), turned(s0, dh))
        outs = [unpack_shard(scatter_call(d0, 1)), unpack_shard(sum1)]
        return (dx[None], *(jnp.stack([o[i] for o in outs]) for i in range(3)))

    cut = P(None, "dp", None)
    return jax.shard_map(
        step, mesh=mesh, in_specs=(P("dp"), P("dp"), cut, cut, cut), out_specs=(P("dp"), cut, cut, cut), check_vma=False
    )
```

```python
import functools

import jax
import jax.numpy as jnp
import numpy as np
from jax import lax
from jax.experimental import pallas as pl
from jax.experimental.pallas import tpu as pltpu
from jax.sharding import PartitionSpec as P

D = 896
FF = 2304
HALF = 112
TOK = 2048
C = FF + 1024
BF = jnp.bfloat16
F32 = jnp.float32
MESH = pl.DeviceIdType.MESH
ALL = slice(None)
GRID = (4, 4, 4, 2, 16)
PACKED = (8, 256, C)
TILE = 128
ORDERS = ((0, 1, 2), (1, 2, 0), (2, 0, 1)) * 2
FRONT, BACK = (0, 1, 2), (3, 4, 5)
ANY = pl.BlockSpec(memory_space=pl.ANY)
VMEM = pl.BlockSpec(memory_space=pltpu.VMEM)


def colours(width):
    tiles = width // 128
    out, at = [], 0
    for count in (tiles // 2, tiles - tiles // 2):
        for k in range(3):
            n = count // 3 + (1 if k < count % 3 else 0)
            first = (n + 1) // 2
            out.append(((at, first * 128), (at + first * 128, (n - first) * 128)))
            at += n * 128
    return out


def where():
    me = lax.axis_index("dp")
    return (me // 32, lax.rem(me // 8, 4), lax.rem(me // 2, 4)), lax.rem(me, 2)


def number(xyz, c):
    return ((xyz[0] * 4 + xyz[1]) * 4 + xyz[2]) * 2 + c


def moved(xyz, axis, by):
    out = list(xyz)
    out[axis] = lax.rem(xyz[axis] + by + 4, 4)
    return tuple(out)


def greet(xyz, c):
    barrier = pltpu.get_barrier_semaphore()
    for axis in range(3):
        for by in (1, -1):
            pl.semaphore_signal(barrier, inc=1, device_id={"dp": number(moved(xyz, axis, by), c)}, device_id_type=MESH)
    pl.semaphore_signal(barrier, inc=1, device_id={"dp": number(xyz, 1 - c)}, device_id_type=MESH)


def greeted():
    pl.semaphore_wait(pltpu.get_barrier_semaphore(), 7)


def remote(src, dst, send, recv, xyz, c):
    return pltpu.make_async_remote_copy(
        src_ref=src, dst_ref=dst, send_sem=send, recv_sem=recv, device_id={"dp": number(xyz, c)}, device_id_type=MESH
    )


POINT = (16, C)
LINE = (4, *POINT)
PLANE = (4, *LINE)
EACH = pltpu.SemaphoreType.DMA((6,))
SEMS = [pltpu.SemaphoreType.DMA((6, 3, 6))] * 2


class Gather:
    def __init__(self, cols, shard, g, send, recv, dsend, drecv, lsem):
        self.cols, self.shard, self.g = cols, shard, g
        self.send, self.recv, self.dsend, self.drecv, self.lsem = send, recv, dsend, drecv, lsem
        self.xyz, self.c = where()
        self.pending, self.partner = [], []

    def at(self, k, phase, by):
        return moved(self.xyz, ORDERS[k][phase], by)

    def block(self, k, phase, by, half, c):
        order, xyz = ORDERS[k], self.at(k, phase, by)
        at = [ALL if axis in order[:phase] else xyz[axis] for axis in range(3)]
        start, size = self.cols[k][half]
        return self.g.at[at[0], at[1], at[2], c, :, pl.ds(start, size)]

    def copy(self, k, phase, owner, half, to, slot):
        here = self.block(k, phase, owner, half, self.c)
        start, size = self.cols[k][half]
        src = self.shard.at[:, pl.ds(start, size)] if phase == 0 and owner == 0 else here
        return remote(src, here, self.send.at[k, phase, slot], self.recv.at[k, phase, slot], self.at(k, phase, to), self.c)

    def local(self):
        return pltpu.make_async_copy(self.shard, self.g.at[self.xyz[0], self.xyz[1], self.xyz[2], self.c], self.lsem)

    def over(self, k, phase, owner, half, slot, c):
        here = self.block(k, phase, owner, half, c)
        return remote(here, here, self.dsend.at[k, slot], self.drecv.at[k, slot], self.xyz, 1 - self.c)

    def go(self, *what):
        self.copy(*what).start()
        self.pending.append(what)

    def give(self, *what):
        self.over(*what, self.c).start()
        self.partner.append(what)

    def begin(self, phase, ks):
        if ks == FRONT and phase == 0:
            self.local().start()
        if ks == FRONT and phase == 1:
            self.local().wait()
        for k in ks:
            for to, half, slot in ((1, 0, 0), (-1, 1, 3), (1, 1, 1), (-1, 0, 2)):
                self.go(k, phase, 0, half, to, slot)
            if phase == 2:
                for half in range(2):
                    self.give(k, 2, 0, half, half)

    def relay(self, phase, ks):
        for k in ks:
            for owner, to, half, slot, out in ((-1, 1, 0, 0, 4), (1, -1, 1, 3, 5)):
                self.copy(k, phase, owner, half, to, slot).wait_recv()
                self.go(k, phase, owner, half, to, out)
                if phase == 2:
                    self.give(k, 2, owner, half, 2 + half)

    def finish(self, phase, ks):
        for k in ks:
            for owner, half, slot, give in ((-1, 1, 1, 4), (1, 0, 2, 5), (2, 0, 4, 6), (2, 1, 5, 7)):
                self.copy(k, phase, owner, half, 1, slot).wait_recv()
                if phase == 2:
                    self.give(k, 2, owner, half, give)

    def end(self):
        for what in self.partner:
            self.over(*what, 1 - self.c).wait_recv()
            self.over(*what, self.c).wait_send()
        for what in self.pending:
            self.copy(*what).wait_send()

    def steps(self, plan):
        out = []
        for name, phase in plan:
            out += [functools.partial(getattr(self, name), phase, ks) for ks in (FRONT, BACK)]
        return out + [self.end]

    def turn(self, phase, ks):
        self.finish(phase - 1, ks)
        self.begin(phase, ks)


GATHER_SEMS = [*SEMS, *[pltpu.SemaphoreType.DMA((6, 8))] * 2, pltpu.SemaphoreType.DMA]


EARLY = (("begin", 0), ("relay", 0), ("turn", 1), ("relay", 1))
LATE = (("relay", 2), ("finish", 2))


def gather_kernel(cols, shard, next_shard, g, next_g, *sems):
    gather, ahead = Gather(cols, shard, g, *sems[:5]), Gather(cols, next_shard, next_g, *sems[5:])
    greet(gather.xyz, gather.c)
    greeted()
    steps = gather.steps(EARLY + (("turn", 2),) + LATE)
    others = ahead.steps(EARLY + (("finish", 1),))
    for n in range(0, len(steps) - 1, 2):
        for step in (*steps[n : n + 2], *others[:-1][n : n + 2]):
            step()
    steps[-1]()
    others[-1]()


def gather_call(shard, next_shard):
    g = jax.ShapeDtypeStruct((*GRID, C), BF)
    return pl.pallas_call(
        functools.partial(gather_kernel, colours(C)),
        out_shape=[g, g],
        in_specs=[VMEM, VMEM],
        out_specs=[ANY, ANY],
        scratch_shapes=GATHER_SEMS * 2,
        compiler_params=params(collective_id=0),
        name="gather",
    )(shard, next_shard)


class Scatter:
    def __init__(self, cols, ds, out, own, pair, keep, one, left2, right2, next_, send, recv, dsend, drecv, lsem):
        self.cols, self.ds, self.out, self.own, self.pair = cols, ds, out, own, pair
        self.keep, self.one, self.l2, self.r2, self.next = keep, one, left2, right2, next_
        self.send, self.recv, self.dsend, self.drecv, self.lsem = send, recv, dsend, drecv, lsem
        self.xyz, self.c = where()
        self.pending = []

    def source_of(self, k, c):
        (start, n0), (_, n1) = self.cols[k]
        d = self.ds[0]
        if start >= d.shape[-1]:
            d, start = self.ds[1], start - d.shape[-1]
        return d.at[:, :, :, c, :, pl.ds(start, n0 + n1)]

    def local(self, k):
        return pltpu.make_async_copy(self.source_of(k, self.c), self.own.at[:, :, :, :, self.both(k)], self.lsem.at[k])

    def swap(self, k):
        there = self.pair.at[:, :, :, :, self.both(k)]
        return remote(self.source_of(k, 1 - self.c), there, self.dsend.at[k], self.drecv.at[k], self.xyz, 1 - self.c)

    def begin_swap(self):
        for k in range(len(self.cols)):
            self.local(k).start()
            self.swap(k).start()

    def cut(self, k, half):
        start, size = self.cols[k][half]
        return pl.ds(start, size)

    def both(self, k):
        (start, n0), (_, n1) = self.cols[k]
        return pl.ds(start, n0 + n1)

    def add_swap(self, k):
        self.local(k).wait()
        self.swap(k).wait_recv()
        at, axis = self.both(k), ORDERS[k][0]
        mine = (*[self.xyz[axis] if a == axis else ALL for a in range(3)], ALL, at)
        self.keep[0][:, :, :, at] = self.own[mine].astype(F32) + self.pair[mine].astype(F32)

        def body(i, _):
            here = (i, ALL, ALL, ALL, at)
            self.own[here] = (self.own[here].astype(F32) + self.pair[here].astype(F32)).astype(BF)
            return 0

        lax.fori_loop(0, 4, body, 0)

    def source(self, k, phase, where_):
        order = ORDERS[k]
        if phase == 0:
            return [where_ if a == order[0] else ALL for a in range(3)]
        if phase == 1:
            rest = [a for a in range(3) if a != order[0]]
            return [where_ if a == order[1] else ALL for a in rest]
        return [where_]

    def buf(self, phase):
        return self.own if phase == 0 else self.next[phase - 1]

    def copy(self, k, phase, half, slot, to, to_at, dst):
        axis = ORDERS[k][phase]
        at, to = moved(self.xyz, axis, to_at)[axis], moved(self.xyz, axis, to)
        src = self.buf(phase).at[(*self.source(k, phase, at), ALL, self.cut(k, half))]
        lead = [ALL] * (2 - phase)
        there = dst[phase].at[(*lead, ALL, self.cut(k, half))]
        return remote(src, there, self.send.at[k, phase, slot], self.recv.at[k, phase, slot], to, self.c)

    def go(self, *what):
        self.copy(*what).start()
        self.pending.append(what)

    def first(self, k, phase):
        self.go(k, phase, 0, 0, 1, 2, self.one)
        self.go(k, phase, 1, 1, -1, 2, self.one)
        self.go(k, phase, 1, 2, 1, 1, self.l2)
        self.go(k, phase, 0, 3, -1, -1, self.r2)

    def second(self, k, phase):
        axis = ORDERS[k][phase]
        for half, slot, to, dst, out in ((0, 0, 1, self.l2, 4), (1, 1, -1, self.r2, 5)):
            self.copy(k, phase, half, slot, to, 2, self.one).wait_recv()
            at, buf = self.cut(k, half), self.buf(phase)
            where_ = self.source(k, phase, moved(self.xyz, axis, to)[axis])

            here = (*where_, ALL, at)
            got = self.one[phase][(*[ALL] * (3 - phase), at)]
            buf[here] = (buf[here].astype(F32) + got.astype(F32)).astype(BF)
            self.go(k, phase, half, out, to, to, dst)

    def third(self, k, phase):
        for half, slot, dst in ((1, 2, self.l2), (0, 3, self.r2), (0, 4, self.l2), (1, 5, self.r2)):
            self.copy(k, phase, half, slot, 1, 1, dst).wait_recv()
        at, order = self.both(k), ORDERS[k]

        def total(*lead):
            here = (*lead, ALL, at)
            return self.keep[phase][here] + self.l2[phase][here].astype(F32) + self.r2[phase][here].astype(F32)

        if phase == 2:
            self.out[:, at] = total().astype(BF)
            return
        rest = [a for a in range(3) if a not in order[:phase] and a != order[phase]]
        everything = [ALL] * len(rest)
        mine = [self.xyz[a] if a == order[phase + 1] else ALL for a in rest]
        self.next[phase][(*everything, ALL, at)] = total(*everything).astype(BF)
        self.keep[phase + 1][(*everything[1:], ALL, at)] = total(*mine)

    def end(self):
        for k in range(len(self.cols) if self.ds else 0):
            self.swap(k).wait_send()
        for what in self.pending:
            self.copy(*what).wait_send()

    def opened(self, ks):
        for k in ks:
            self.add_swap(k)
            self.first(k, 0)

    def seconds(self, phase, ks):
        for k in ks:
            self.second(k, phase)

    def thirds(self, phase, ks, on=True):
        for k in ks:
            self.third(k, phase)
            if on and phase < 2:
                self.first(k, phase + 1)

    def resume(self, ks):
        for k in ks:
            self.first(k, 1)

    def steps_first(self):
        out = [self.begin_swap]
        for f in (self.opened, functools.partial(self.seconds, 0), functools.partial(self.thirds, 0, on=False)):
            out += [functools.partial(f, ks) for ks in (FRONT, BACK)]
        return out + [self.end]

    def steps_rest(self):
        out = [functools.partial(self.resume, FRONT + BACK)]
        for phase in (1, 2):
            out += [functools.partial(f, phase, FRONT + BACK) for f in (self.seconds, self.thirds)]
        return out + [self.end]

    def steps(self):
        groups = (FRONT, BACK)[: len(self.cols) // 3]
        out = [self.begin_swap]
        out += [functools.partial(self.opened, ks) for ks in groups]
        for phase in range(3):
            out += [functools.partial(self.seconds, phase, ks) for ks in groups]
            out += [functools.partial(self.thirds, phase, ks) for ks in groups]
        return out + [self.end]


def shares():
    cols, at = [], 0
    for n in (5, 5, 4, 4, 4, 4):
        first = (n + 1) // 2 * 128
        cols.append(((at, first), (at + first, n * 128 - first)))
        at += n * 128
    return cols


def scatter_of(ds, out, scratch):
    buffers = [scratch[2 + 3 * n : 5 + 3 * n] for n in range(4)]
    return Scatter(shares(), ds, out, *scratch[:2], *buffers, scratch[14:16], *scratch[16:])


def scatter_first(ds, rounded, kept, scratch):
    own, pair, keep, one, left2, right2, *sems = scratch
    return Scatter(shares(), ds, None, own, pair, (keep, kept), (one,), (left2,), (right2,), (rounded,), *sems)


def scatter_rest(rounded, kept, out, scratch):
    keep, one, left2, right2, next_, *sems = scratch[0], scratch[1:3], scratch[3:5], scratch[5:7], scratch[7], *scratch[8:]
    buffers = [(None, *t) for t in (one, left2, right2)]
    return Scatter(shares(), None, out, None, None, (None, kept, keep), *buffers, (rounded, next_), *sems, None, None, None)


CUBE = [pltpu.VMEM((4, *PLANE), BF)] * 2
FIRST = [*CUBE, pltpu.VMEM(PLANE, F32), *[pltpu.VMEM(PLANE, BF)] * 3, *SEMS, *[EACH] * 3]
REST = [pltpu.VMEM(POINT, F32), *[pltpu.VMEM(LINE, BF), pltpu.VMEM(POINT, BF)] * 3, pltpu.VMEM(LINE, BF), *SEMS]
WHOLE = [
    *CUBE,
    *[pltpu.VMEM(t, F32) for t in (PLANE, LINE, POINT)],
    *[pltpu.VMEM(t, BF) for t in (PLANE, LINE, POINT) * 3],
    pltpu.VMEM(PLANE, BF), pltpu.VMEM(LINE, BF), *SEMS, *[EACH] * 3,
]


def picks():
    gu = np.zeros((224, 256), np.float32)
    down = np.zeros((288, 288), np.float32)
    last = np.zeros((224, 256), np.float32)
    for d in range(16):
        for j in range(7):
            gu[7 * d + j, 16 * d + j] = 1
            gu[112 + 7 * d + j, 16 * d + 8 + j] = 1
        for r in range(16):
            down[18 * d + r, 16 * d + r] = 1
        for e in range(2):
            down[18 * d + 16 + e, 256 + 16 * e + d] = 1
            for t in range(7):
                last[32 * t + 16 * e + d, 16 * d + 7 * e + t] = 1
    return tuple(jnp.asarray(t, BF) for t in (gu, down, last))


def pack_shard(gate, up, down):
    zero = jnp.zeros((1, FF), BF)
    gu = jnp.concatenate([gate, zero, up, zero])
    rest = jnp.concatenate([down[16:].reshape(14, TILE), zero[:, : 2 * TILE].reshape(2, TILE)])
    return jnp.concatenate([gu, jnp.concatenate([down[:16], rest], 1)], 1)


def unpack_shard(p):
    down = p[:, FF:]
    return p[:7, :FF], p[8:15, :FF], jnp.concatenate([down[:, :D], down[:14, D:].reshape(2, D)], 0)


def whole(shape):
    return pl.BlockSpec(shape, lambda i: (0,) * len(shape), pipeline_mode=pl.Buffered(1))


def rows(n, width):
    return pl.BlockSpec((n, width), lambda i: (i, 0))


def columns(height, n):
    return pl.BlockSpec((height, n), lambda i: (0, i))


def like(n, width, dtype=BF):
    return jax.ShapeDtypeStruct((n, width), dtype)


def params(**more):
    return pltpu.CompilerParams(vmem_limit_bytes=65011712, has_side_effects=bool(more), **more)


PICKS = [whole((224, 256)), whole((288, 288)), whole((224, 256))]


CHUNK = 768
CHUNKS = tuple(slice(at, at + CHUNK) for at in range(0, FF, CHUNK))


def mm(a, w):
    return lax.dot_general(a, w, (((1,), (0,)), ((), ())), preferred_element_type=F32)


def mmt(a, w):
    return lax.dot_general(a, w, (((1,), (1,)), ((), ())), preferred_element_type=F32)


def norm(h):
    wide = h.astype(F32)
    scale = lax.rsqrt(jnp.mean(wide * wide, -1, keepdims=True) + 1e-6)
    return wide, scale


def norm_back(wide, scale, da, dh):
    da = da.astype(BF).astype(F32)
    inner = jnp.mean(da * wide, -1, keepdims=True)
    by_h = (da * scale - wide * (scale * scale * scale * inner)).astype(BF)
    return (dh.astype(F32) + by_h.astype(F32)).astype(BF)


def sigmoid(g):
    return 1.0 / (1.0 + jnp.exp(-g))


def gated(g, u):
    sig = sigmoid(g)
    soft = g * sig
    return soft, u * (sig * (1.0 + g - soft))


def step_number():
    return pl.program_id(0)


class Ticks:
    def __init__(self, transfer, steps, times, per):
        def start():
            greet(transfer.xyz, transfer.c)
            greeted()
            steps[0]()

        self.steps, self.per, self.times = [start, *steps[1:]], per, times

    def __call__(self, slot):
        for step, time in zip(self.steps, self.times, strict=True):
            if time % self.per == slot:
                pl.when(step_number() == time // self.per)(step)


GATHER_AT = (0, 0, 5, 9, 13, 18, 31)
FIRST_AT = (0, 4, 7, 9, 11, 17, 20, 25)
BOTH_AT = (0, 0, 4, 5, 6, 7, 8, 9, 10, 11, 12, 14, *[15] * 10)


def unpack_all(g, picked, wg, wu, wd):
    gu, down, last = picked

    def body(n, _):
        both = mm(gu[ALL], g[n, :, :FF]).astype(BF)
        at = pl.ds(pl.multiple_of(HALF * n, 16), HALF)
        wg[at, :] = both[:HALF]
        wu[at, :] = both[HALF:]
        ends = mm(last[ALL], g[n, :, FF + D :]).astype(BF)
        ends = jnp.concatenate([ends[32 * t : 32 * t + 32] for t in range(7)], 1)
        packed = jnp.concatenate([g[n, :, FF : FF + D], ends], 0)
        wd[pl.ds(pl.multiple_of(288 * n, 16), 288), :] = mm(down[ALL], packed).astype(BF)
        return 0

    lax.fori_loop(0, 8, body, 0)


WEIGHTS = [pltpu.VMEM((D, FF), BF), pltpu.VMEM((D, FF), BF), pltpu.VMEM((FF, D), BF)]


def forward_kernel(x, g, *rest):
    picked, (_, h, a_out, slope_out, soft_out, s_out, gathered), rest = rest[:3], rest[3:10], rest[10:]
    saved, s, (wg, wu, wd), save_sem, sems = rest[:3], rest[3], rest[4:7], rest[7], rest[8:]
    gather = Gather(colours(C), None, gathered, *sems)
    tick = Ticks(gather, gather.steps((("begin", 2),) + LATE), GATHER_AT, 4)
    saves = [pltpu.make_async_copy(w, out, save_sem.at[n]) for n, (w, out) in enumerate(zip((wg, wu, wd), saved))]
    tick(0)

    @pl.when(step_number() == 0)
    def _():
        unpack_all(g, picked, wg, wu, wd)
        for save in saves:
            save.start()

    wide, scale = norm(x[ALL])
    a = (wide * scale).astype(BF)
    a_out[ALL] = a.T
    for n, at in enumerate(CHUNKS):
        gate, up = mm(a, wg[:, at]), mm(a, wu[:, at])
        soft, slope = gated(gate, up)
        slope_out[:, at] = slope
        soft_out[:, at] = soft
        s[:, at] = (soft * up).astype(BF)
        s_out[at, :] = s[:, at].T
        if n < 2:
            tick(n + 1)
    h[ALL] = (x[ALL].astype(F32) + mm(s[ALL], wd[ALL]).astype(BF).astype(F32)).astype(BF)
    tick(3)

    @pl.when(step_number() == 7)
    def _():
        for save in saves:
            save.wait()


def forward(x, g, part):
    n = TOK // 8
    return pl.pallas_call(
        forward_kernel,
        grid=(8,),
        in_specs=[rows(n, D), whole(PACKED), *PICKS, ANY],
        out_specs=[rows(n, D), columns(D, n), rows(n, FF), rows(n, FF), columns(FF, n), ANY, ANY, ANY, ANY],
        out_shape=[
            like(TOK, D), like(D, TOK), like(TOK, FF, F32), like(TOK, FF, F32), like(FF, TOK),
            jax.ShapeDtypeStruct(part.shape, BF), like(D, FF), like(D, FF), like(FF, D),
        ],
        scratch_shapes=[pltpu.VMEM((n, FF), BF), *WEIGHTS, pltpu.SemaphoreType.DMA((3,)), *GATHER_SEMS],
        input_output_aliases={5: 5},
        compiler_params=params(collective_id=2),
        name="forward",
    )(x, g.reshape(PACKED), *picks(), part)


def middle_kernel(h, dy, slope0, soft0, wd0, g, gu, down, last, a_out, s_out, dg_out, du_out, dh, dg0, du0, wg, wu, wd):
    @pl.when(step_number() == 0)
    def _():
        unpack_all(g, (gu, down, last), wg, wu, wd)

    wide, scale = norm(h[ALL])
    a = (wide * scale).astype(BF)
    a_out[ALL] = a.T
    for at in CHUNKS:
        gate, up = mm(a, wg[:, at]), mm(a, wu[:, at])
        ds = mmt(dy[ALL], wd[at, :]).astype(BF).astype(F32)
        soft, slope = gated(gate, up)
        s_out[at, :] = (soft * up).astype(BF).T
        dg_out[:, at] = (ds * slope).astype(BF)
        du_out[:, at] = (ds * soft).astype(BF)
    da = mmt(dg_out[ALL], wg[ALL]) + mmt(du_out[ALL], wu[ALL])
    by_h = norm_back(wide, scale, da, dy[ALL])
    dh[ALL] = by_h
    for at in CHUNKS:
        ds = mmt(by_h, wd0[at, :]).astype(BF).astype(F32)
        dg0[:, at] = (ds * slope0[:, at]).astype(BF)
        du0[:, at] = (ds * soft0[:, at]).astype(BF)


def middle(h, dy, slope, soft, wd, g):
    n = TOK // 8
    token, wide = rows(n, D), rows(n, FF)
    return pl.pallas_call(
        middle_kernel,
        grid=(8,),
        in_specs=[token, token, wide, wide, whole((FF, D)), whole(PACKED), *PICKS],
        out_specs=[columns(D, n), columns(FF, n), wide, wide, token, wide, wide],
        out_shape=[like(D, TOK), like(FF, TOK), like(TOK, FF), like(TOK, FF), like(TOK, D), like(TOK, FF), like(TOK, FF)],
        scratch_shapes=WEIGHTS,
        compiler_params=params(),
        name="middle",
    )(h, dy, slope, soft, wd, g.reshape(PACKED), *picks())


WIDE = 256
DOWN = 4
UP = FF // WIDE


def early(i):
    return jnp.minimum(i, DOWN - 1)


def late(i):
    return jnp.maximum(i - DOWN, 0)


def down_step(st, dy, down, last, out):
    w = mm(st[ALL], dy[ALL]).astype(BF)
    for n in range(2):
        packed = mm(down[ALL], w[288 * n : 288 * n + 288]).astype(BF)
        out[n, :, :D] = packed[:256]
        ends = jnp.concatenate([packed[256:, 128 * t : 128 * t + 128] for t in range(7)], 0)
        out[n, :, D:] = mm(last[ALL], ends).astype(BF)


def gate_up_step(at, dg, du, gu, out):
    wg = mm(at[ALL], dg[ALL]).astype(BF)
    wu = mm(at[ALL], du[ALL]).astype(BF)
    for n in range(8):
        cut = slice(HALF * n, HALF * n + HALF)
        out[n] = mm(gu[ALL], jnp.concatenate([wg[cut], wu[cut]], 0)).astype(BF)


DOWN_IN = [pl.BlockSpec((576, TOK), lambda i: (early(i), 0)), whole((TOK, D)), whole((288, 288)), whole((256, 224))]
DOWN_OUT = pl.BlockSpec((2, 256, 1024), lambda i: (early(i), 0, 0))


def by_packed(width):
    return jax.ShapeDtypeStruct((8, 256, width), BF)


def split(packed):
    return packed.reshape(*GRID, packed.shape[-1])


SUMMED = whole(POINT)


def weights_kernel(st, dy, down, last, at, dg, du, gu, *rest, reduce):
    tick = lambda slot: None
    if reduce:
        *before, down_out, gu_out, rounded, kept = rest[:6]
        scatter = scatter_first(before, rounded, kept, rest[6:])
        tick = Ticks(scatter, scatter.steps_first(), FIRST_AT, 2)
    else:
        down_out, gu_out = rest
    tick(0)
    pl.when(step_number() < DOWN)(lambda: down_step(st, dy, down, last, down_out))
    pl.when(step_number() >= DOWN)(lambda: gate_up_step(at, dg, du, gu, gu_out))
    tick(1)


def by_weights(st, dy, at, dg, du, before=()):
    gu, down, last = picks()
    tile = pl.BlockSpec((TOK, WIDE), lambda i: (0, late(i)))
    more = bool(before)
    by_down, by_gu, *out = pl.pallas_call(
        functools.partial(weights_kernel, reduce=more),
        grid=(DOWN + UP,),
        in_specs=[*DOWN_IN, whole((D, TOK)), tile, tile, whole((256, 224)), *[ANY for _ in before]],
        out_specs=[DOWN_OUT, pl.BlockSpec((8, 256, WIDE), lambda i: (0, 0, late(i))), *[whole(PLANE), whole(LINE)] * more],
        out_shape=[by_packed(1024), by_packed(FF), *[jax.ShapeDtypeStruct(PLANE, BF), jax.ShapeDtypeStruct(LINE, F32)] * more],
        scratch_shapes=FIRST * more,
        compiler_params=params(**(dict(collective_id=4) if more else {})),
        name="by_weights",
    )(st, dy, down.T, last.T, at, dg, du, gu.T, *before)
    return split(by_gu), split(by_down), *out


def backward_kernel(x, dh, dg, du, wg, wu, by_gu, by_down, rounded, kept, dx, out0, out1, *scratch):
    ahead = scatter_rest(scratch[0], kept, out1, scratch[1 : 1 + len(REST)])
    scatter = scatter_of((by_gu, by_down), out0, scratch[1 + len(REST) :])

    def resume():
        scratch[0][ALL] = rounded[ALL]
        others[0]()

    steps, others = scatter.steps(), ahead.steps_rest()
    mixed = [t for pair in zip(steps, [resume, *others[1:-1]]) for t in pair]
    tick = Ticks(scatter, [*mixed, *steps[len(others) - 1 :], others[-1]], BOTH_AT, 2)
    tick(0)
    wide, scale = norm(x[ALL])
    da = mmt(dg[ALL], wg[ALL]) + mmt(du[ALL], wu[ALL])
    dx[ALL] = norm_back(wide, scale, da, dh[ALL])
    tick(1)


def backward(x, dh, dg, du, wg, wu, before):
    n = TOK // 8
    return pl.pallas_call(
        backward_kernel,
        grid=(8,),
        in_specs=[
            rows(n, D), rows(n, D), rows(n, FF), rows(n, FF), whole((D, FF)), whole((D, FF)), ANY, ANY, whole(PLANE), whole(LINE),
        ],
        out_specs=[rows(n, D), SUMMED, SUMMED],
        out_shape=[like(TOK, D), like(*POINT), like(*POINT)],
        scratch_shapes=[pltpu.VMEM(PLANE, BF), *REST, *WHOLE],
        compiler_params=params(collective_id=3),
        name="backward",
    )(x, dh, dg, du, wg, wu, *before)


def solution(mesh):
    def step(x, dy, gate, up, down):
        x, dy = x[0], dy[0]
        part0, part1 = gather_call(*[pack_shard(gate[n], up[n], down[n]) for n in range(2)])
        h, a0, slope, soft, s0, part1, wg, wu, wd = forward(x, part0, part1)
        a1, s1, dg1, du1, dh, dg, du = middle(h, dy, slope, soft, wd, part1)
        before = by_weights(s1, dy, a1, dg1, du1)
        before = by_weights(s0, dh, a0, dg, du, before)
        dx, sum0, sum1 = backward(x, dh, dg, du, wg, wu, before)
        outs = [unpack_shard(t) for t in (sum0, sum1)]
        return (dx[None], *(jnp.stack([o[i] for o in outs]) for i in range(3)))

    cut = P(None, "dp", None)
    return jax.shard_map(
        step, mesh=mesh, in_specs=(P("dp"), P("dp"), cut, cut, cut), out_specs=(P("dp"), cut, cut, cut), check_vma=False
    )
```

```python
import functools

import jax
import jax.numpy as jnp
import numpy as np
from jax import lax
from jax.experimental import pallas as pl
from jax.experimental.pallas import tpu as pltpu
from jax.sharding import PartitionSpec as P

D = 896
FF = 2304
HALF = 112
TOK = 2048
C = FF + 1024
BF = jnp.bfloat16
F32 = jnp.float32
MESH = pl.DeviceIdType.MESH
ALL = slice(None)
GRID = (4, 4, 4, 2, 16)
PACKED = (8, 256, C)
TILE = 128
ORDERS = ((0, 1, 2), (1, 2, 0), (2, 0, 1)) * 2
FRONT, BACK = (0, 1, 2), (3, 4, 5)
ANY = pl.BlockSpec(memory_space=pl.ANY)
VMEM = pl.BlockSpec(memory_space=pltpu.VMEM)


def colours(width):
    tiles = width // 128
    out, at = [], 0
    for count in (tiles // 2, tiles - tiles // 2):
        for k in range(3):
            n = count // 3 + (1 if k < count % 3 else 0)
            first = (n + 1) // 2
            out.append(((at, first * 128), (at + first * 128, (n - first) * 128)))
            at += n * 128
    return out


def where():
    me = lax.axis_index("dp")
    return (me // 32, lax.rem(me // 8, 4), lax.rem(me // 2, 4)), lax.rem(me, 2)


def number(xyz, c):
    return ((xyz[0] * 4 + xyz[1]) * 4 + xyz[2]) * 2 + c


def moved(xyz, axis, by):
    out = list(xyz)
    out[axis] = lax.rem(xyz[axis] + by + 4, 4)
    return tuple(out)


def greet(xyz, c):
    barrier = pltpu.get_barrier_semaphore()
    for axis in range(3):
        for by in (1, -1):
            pl.semaphore_signal(barrier, inc=1, device_id={"dp": number(moved(xyz, axis, by), c)}, device_id_type=MESH)
    pl.semaphore_signal(barrier, inc=1, device_id={"dp": number(xyz, 1 - c)}, device_id_type=MESH)


def greeted():
    pl.semaphore_wait(pltpu.get_barrier_semaphore(), 7)


def remote(src, dst, send, recv, xyz, c):
    return pltpu.make_async_remote_copy(
        src_ref=src, dst_ref=dst, send_sem=send, recv_sem=recv, device_id={"dp": number(xyz, c)}, device_id_type=MESH
    )


POINT = (16, C)
LINE = (4, *POINT)
PLANE = (4, *LINE)
EACH = pltpu.SemaphoreType.DMA((6,))
SEMS = [pltpu.SemaphoreType.DMA((6, 3, 6))] * 2


class Gather:
    def __init__(self, cols, shard, g, send, recv, dsend, drecv, lsem):
        self.cols, self.shard, self.g = cols, shard, g
        self.send, self.recv, self.dsend, self.drecv, self.lsem = send, recv, dsend, drecv, lsem
        self.xyz, self.c = where()
        self.pending, self.partner = [], []

    def at(self, k, phase, by):
        return moved(self.xyz, ORDERS[k][phase], by)

    def block(self, k, phase, by, half, c):
        order, xyz = ORDERS[k], self.at(k, phase, by)
        at = [ALL if axis in order[:phase] else xyz[axis] for axis in range(3)]
        start, size = self.cols[k][half]
        return self.g.at[at[0], at[1], at[2], c, :, pl.ds(start, size)]

    def copy(self, k, phase, owner, half, to, slot):
        here = self.block(k, phase, owner, half, self.c)
        start, size = self.cols[k][half]
        src = self.shard.at[:, pl.ds(start, size)] if phase == 0 and owner == 0 else here
        return remote(src, here, self.send.at[k, phase, slot], self.recv.at[k, phase, slot], self.at(k, phase, to), self.c)

    def local(self):
        return pltpu.make_async_copy(self.shard, self.g.at[self.xyz[0], self.xyz[1], self.xyz[2], self.c], self.lsem)

    def over(self, k, phase, owner, half, slot, c):
        here = self.block(k, phase, owner, half, c)
        return remote(here, here, self.dsend.at[k, slot], self.drecv.at[k, slot], self.xyz, 1 - self.c)

    def go(self, *what):
        self.copy(*what).start()
        self.pending.append(what)

    def give(self, *what):
        self.over(*what, self.c).start()
        self.partner.append(what)

    def begin(self, phase, ks):
        if ks == FRONT and phase == 0:
            self.local().start()
        if ks == FRONT and phase == 1:
            self.local().wait()
        for k in ks:
            for to, half, slot in ((1, 0, 0), (-1, 1, 3), (1, 1, 1), (-1, 0, 2)):
                self.go(k, phase, 0, half, to, slot)
            if phase == 2:
                for half in range(2):
                    self.give(k, 2, 0, half, half)

    def relay(self, phase, ks):
        for k in ks:
            for owner, to, half, slot, out in ((-1, 1, 0, 0, 4), (1, -1, 1, 3, 5)):
                self.copy(k, phase, owner, half, to, slot).wait_recv()
                self.go(k, phase, owner, half, to, out)
                if phase == 2:
                    self.give(k, 2, owner, half, 2 + half)

    def finish(self, phase, ks):
        for k in ks:
            for owner, half, slot, give in ((-1, 1, 1, 4), (1, 0, 2, 5), (2, 0, 4, 6), (2, 1, 5, 7)):
                self.copy(k, phase, owner, half, 1, slot).wait_recv()
                if phase == 2:
                    self.give(k, 2, owner, half, give)

    def end(self):
        for what in self.partner:
            self.over(*what, 1 - self.c).wait_recv()
            self.over(*what, self.c).wait_send()
        for what in self.pending:
            self.copy(*what).wait_send()

    def steps(self, plan):
        out = []
        for name, phase in plan:
            out += [functools.partial(getattr(self, name), phase, ks) for ks in (FRONT, BACK)]
        return out + [self.end]

    def turn(self, phase, ks):
        self.finish(phase - 1, ks)
        self.begin(phase, ks)


GATHER_SEMS = [*SEMS, *[pltpu.SemaphoreType.DMA((6, 8))] * 2, pltpu.SemaphoreType.DMA]


EARLY = (("begin", 0), ("relay", 0), ("turn", 1), ("relay", 1))
LATE = (("relay", 2), ("finish", 2))


def gather_kernel(cols, shard, next_shard, g, next_g, *sems):
    gather, ahead = Gather(cols, shard, g, *sems[:5]), Gather(cols, next_shard, next_g, *sems[5:])
    greet(gather.xyz, gather.c)
    greeted()
    steps = gather.steps(EARLY + (("turn", 2),) + LATE)
    others = ahead.steps(EARLY + (("finish", 1),))
    for n in range(0, len(steps) - 1, 2):
        for step in (*steps[n : n + 2], *others[:-1][n : n + 2]):
            step()
    steps[-1]()
    others[-1]()


def gather_call(shard, next_shard):
    g = jax.ShapeDtypeStruct((*GRID, C), BF)
    return pl.pallas_call(
        functools.partial(gather_kernel, colours(C)),
        out_shape=[g, g],
        in_specs=[VMEM, VMEM],
        out_specs=[ANY, ANY],
        scratch_shapes=GATHER_SEMS * 2,
        compiler_params=params(collective_id=0),
        name="gather",
    )(shard, next_shard)


class Scatter:
    def __init__(self, cols, ds, out, own, pair, keep, one, left2, right2, next_, send, recv, dsend, drecv, lsem):
        self.cols, self.ds, self.out, self.own, self.pair = cols, ds, out, own, pair
        self.keep, self.one, self.l2, self.r2, self.next = keep, one, left2, right2, next_
        self.send, self.recv, self.dsend, self.drecv, self.lsem = send, recv, dsend, drecv, lsem
        self.xyz, self.c = where()
        self.pending = []

    def source_of(self, k, c):
        (start, n0), (_, n1) = self.cols[k]
        d = self.ds[0]
        if start >= d.shape[-1]:
            d, start = self.ds[1], start - d.shape[-1]
        return d.at[:, :, :, c, :, pl.ds(start, n0 + n1)]

    def local(self, k):
        return pltpu.make_async_copy(self.source_of(k, self.c), self.own.at[:, :, :, :, self.both(k)], self.lsem.at[k])

    def swap(self, k):
        there = self.pair.at[:, :, :, :, self.both(k)]
        return remote(self.source_of(k, 1 - self.c), there, self.dsend.at[k], self.drecv.at[k], self.xyz, 1 - self.c)

    def begin_swap(self):
        for k in range(len(self.cols)):
            self.local(k).start()
            self.swap(k).start()

    def cut(self, k, half):
        start, size = self.cols[k][half]
        return pl.ds(start, size)

    def both(self, k):
        (start, n0), (_, n1) = self.cols[k]
        return pl.ds(start, n0 + n1)

    def add_swap(self, k):
        self.local(k).wait()
        self.swap(k).wait_recv()
        at, axis = self.both(k), ORDERS[k][0]
        mine = (*[self.xyz[axis] if a == axis else ALL for a in range(3)], ALL, at)
        self.keep[0][:, :, :, at] = self.own[mine].astype(F32) + self.pair[mine].astype(F32)

        def body(i, _):
            here = (i, ALL, ALL, ALL, at)
            self.own[here] = (self.own[here].astype(F32) + self.pair[here].astype(F32)).astype(BF)
            return 0

        lax.fori_loop(0, 4, body, 0)

    def source(self, k, phase, where_):
        order = ORDERS[k]
        if phase == 0:
            return [where_ if a == order[0] else ALL for a in range(3)]
        if phase == 1:
            rest = [a for a in range(3) if a != order[0]]
            return [where_ if a == order[1] else ALL for a in rest]
        return [where_]

    def buf(self, phase):
        return self.own if phase == 0 else self.next[phase - 1]

    def copy(self, k, phase, half, slot, to, to_at, dst):
        axis = ORDERS[k][phase]
        at, to = moved(self.xyz, axis, to_at)[axis], moved(self.xyz, axis, to)
        src = self.buf(phase).at[(*self.source(k, phase, at), ALL, self.cut(k, half))]
        lead = [ALL] * (2 - phase)
        there = dst[phase].at[(*lead, ALL, self.cut(k, half))]
        return remote(src, there, self.send.at[k, phase, slot], self.recv.at[k, phase, slot], to, self.c)

    def go(self, *what):
        self.copy(*what).start()
        self.pending.append(what)

    def first(self, k, phase):
        self.go(k, phase, 0, 0, 1, 2, self.one)
        self.go(k, phase, 1, 1, -1, 2, self.one)
        self.go(k, phase, 1, 2, 1, 1, self.l2)
        self.go(k, phase, 0, 3, -1, -1, self.r2)

    def second(self, k, phase):
        axis = ORDERS[k][phase]
        for half, slot, to, dst, out in ((0, 0, 1, self.l2, 4), (1, 1, -1, self.r2, 5)):
            self.copy(k, phase, half, slot, to, 2, self.one).wait_recv()
            at, buf = self.cut(k, half), self.buf(phase)
            where_ = self.source(k, phase, moved(self.xyz, axis, to)[axis])

            here = (*where_, ALL, at)
            got = self.one[phase][(*[ALL] * (3 - phase), at)]
            buf[here] = (buf[here].astype(F32) + got.astype(F32)).astype(BF)
            self.go(k, phase, half, out, to, to, dst)

    def third(self, k, phase):
        for half, slot, dst in ((1, 2, self.l2), (0, 3, self.r2), (0, 4, self.l2), (1, 5, self.r2)):
            self.copy(k, phase, half, slot, 1, 1, dst).wait_recv()
        at, order = self.both(k), ORDERS[k]

        def total(*lead):
            here = (*lead, ALL, at)
            return self.keep[phase][here] + self.l2[phase][here].astype(F32) + self.r2[phase][here].astype(F32)

        if phase == 2:
            self.out[:, at] = total().astype(BF)
            return
        rest = [a for a in range(3) if a not in order[:phase] and a != order[phase]]
        everything = [ALL] * len(rest)
        mine = [self.xyz[a] if a == order[phase + 1] else ALL for a in rest]
        self.next[phase][(*everything, ALL, at)] = total(*everything).astype(BF)
        self.keep[phase + 1][(*everything[1:], ALL, at)] = total(*mine)

    def end(self):
        for k in range(len(self.cols) if self.ds else 0):
            self.swap(k).wait_send()
        for what in self.pending:
            self.copy(*what).wait_send()

    def opened(self, ks):
        for k in ks:
            self.add_swap(k)
            self.first(k, 0)

    def seconds(self, phase, ks):
        for k in ks:
            self.second(k, phase)

    def thirds(self, phase, ks, on=True):
        for k in ks:
            self.third(k, phase)
            if on and phase < 2:
                self.first(k, phase + 1)

    def resume(self, ks):
        for k in ks:
            self.first(k, 1)

    def steps_first(self):
        out = [self.begin_swap]
        for f in (self.opened, functools.partial(self.seconds, 0), functools.partial(self.thirds, 0, on=False)):
            out += [functools.partial(f, ks) for ks in (FRONT, BACK)]
        return out + [self.end]

    def steps_rest(self):
        out = [functools.partial(self.resume, FRONT + BACK)]
        for phase in (1, 2):
            out += [functools.partial(f, phase, FRONT + BACK) for f in (self.seconds, self.thirds)]
        return out + [self.end]

    def steps(self):
        groups = (FRONT, BACK)[: len(self.cols) // 3]
        out = [self.begin_swap]
        out += [functools.partial(self.opened, ks) for ks in groups]
        for phase in range(3):
            out += [functools.partial(self.seconds, phase, ks) for ks in groups]
            out += [functools.partial(self.thirds, phase, ks) for ks in groups]
        return out + [self.end]


def shares():
    cols, at = [], 0
    for n in (5, 5, 4, 4, 4, 4):
        first = (n + 1) // 2 * 128
        cols.append(((at, first), (at + first, n * 128 - first)))
        at += n * 128
    return cols


def scatter_of(ds, out, scratch):
    buffers = [scratch[2 + 3 * n : 5 + 3 * n] for n in range(4)]
    return Scatter(shares(), ds, out, *scratch[:2], *buffers, scratch[14:16], *scratch[16:])


def scatter_first(ds, rounded, kept, scratch):
    own, pair, keep, one, left2, right2, *sems = scratch
    return Scatter(shares(), ds, None, own, pair, (keep, kept), (one,), (left2,), (right2,), (rounded,), *sems)


def scatter_rest(rounded, kept, out, scratch):
    keep, one, left2, right2, next_, *sems = scratch[0], scratch[1:3], scratch[3:5], scratch[5:7], scratch[7], *scratch[8:]
    buffers = [(None, *t) for t in (one, left2, right2)]
    return Scatter(shares(), None, out, None, None, (None, kept, keep), *buffers, (rounded, next_), *sems, None, None, None)


CUBE = [pltpu.VMEM((4, *PLANE), BF)] * 2
FIRST = [*CUBE, pltpu.VMEM(PLANE, F32), *[pltpu.VMEM(PLANE, BF)] * 3, *SEMS, *[EACH] * 3]
REST = [pltpu.VMEM(POINT, F32), *[pltpu.VMEM(LINE, BF), pltpu.VMEM(POINT, BF)] * 3, pltpu.VMEM(LINE, BF), *SEMS]
WHOLE = [
    *CUBE,
    *[pltpu.VMEM(t, F32) for t in (PLANE, LINE, POINT)],
    *[pltpu.VMEM(t, BF) for t in (PLANE, LINE, POINT) * 3],
    pltpu.VMEM(PLANE, BF), pltpu.VMEM(LINE, BF), *SEMS, *[EACH] * 3,
]


def picks():
    gu = np.zeros((224, 256), np.float32)
    down = np.zeros((288, 288), np.float32)
    last = np.zeros((224, 256), np.float32)
    for d in range(16):
        for j in range(7):
            gu[7 * d + j, 16 * d + j] = 1
            gu[112 + 7 * d + j, 16 * d + 8 + j] = 1
        for r in range(16):
            down[18 * d + r, 16 * d + r] = 1
        for e in range(2):
            down[18 * d + 16 + e, 256 + 16 * e + d] = 1
            for t in range(7):
                last[32 * t + 16 * e + d, 16 * d + 7 * e + t] = 1
    return tuple(jnp.asarray(t, BF) for t in (gu, down, last))


def pack_shard(gate, up, down):
    zero = jnp.zeros((1, FF), BF)
    gu = jnp.concatenate([gate, zero, up, zero])
    rest = jnp.concatenate([down[16:].reshape(14, TILE), zero[:, : 2 * TILE].reshape(2, TILE)])
    return jnp.concatenate([gu, jnp.concatenate([down[:16], rest], 1)], 1)


def unpack_shard(p):
    down = p[:, FF:]
    return p[:7, :FF], p[8:15, :FF], jnp.concatenate([down[:, :D], down[:14, D:].reshape(2, D)], 0)


def whole(shape):
    return pl.BlockSpec(shape, lambda i: (0,) * len(shape), pipeline_mode=pl.Buffered(1))


def rows(n, width):
    return pl.BlockSpec((n, width), lambda i: (i, 0))


def columns(height, n):
    return pl.BlockSpec((height, n), lambda i: (0, i))


def like(n, width, dtype=BF):
    return jax.ShapeDtypeStruct((n, width), dtype)


def params(**more):
    return pltpu.CompilerParams(vmem_limit_bytes=65011712, has_side_effects=bool(more), **more)


PICKS = [whole((224, 256)), whole((288, 288)), whole((224, 256))]


CHUNK = 768
CHUNKS = tuple(slice(at, at + CHUNK) for at in range(0, FF, CHUNK))


def mm(a, w):
    return lax.dot_general(a, w, (((1,), (0,)), ((), ())), preferred_element_type=F32)


def mmt(a, w):
    return lax.dot_general(a, w, (((1,), (1,)), ((), ())), preferred_element_type=F32)


def norm(h):
    wide = h.astype(F32)
    scale = lax.rsqrt(jnp.mean(wide * wide, -1, keepdims=True) + 1e-6)
    return wide, scale


def norm_back(wide, scale, da, dh):
    da = da.astype(BF).astype(F32)
    inner = jnp.mean(da * wide, -1, keepdims=True)
    by_h = (da * scale - wide * (scale * scale * scale * inner)).astype(BF)
    return (dh.astype(F32) + by_h.astype(F32)).astype(BF)


def sigmoid(g):
    return 1.0 / (1.0 + jnp.exp(-g))


def gated(g, u):
    sig = sigmoid(g)
    soft = g * sig
    return soft, u * (sig * (1.0 + g - soft))


def step_number():
    return pl.program_id(0)


class Ticks:
    def __init__(self, transfer, steps, times, per):
        def start():
            greeted()
            steps[0]()

        pl.when(step_number() == 0)(lambda: greet(transfer.xyz, transfer.c))
        self.steps, self.per, self.times = [start, *steps[1:]], per, times

    def __call__(self, slot):
        for step, time in zip(self.steps, self.times, strict=True):
            if time % self.per == slot:
                pl.when(step_number() == time // self.per)(step)


GATHER_AT = (0, 0, 12, 16, 20, 25, 31)
FIRST_AT = (2, 6, 9, 11, 13, 19, 22, 25)
BOTH_AT = (2, 2, 5, 6, 7, 8, 9, 10, 11, 12, 13, 14, *[15] * 10)


def unpack_all(g, picked, wg, wu, wd):
    gu, down, last = picked

    def body(n, _):
        both = mm(gu[ALL], g[n, :, :FF]).astype(BF)
        at = pl.ds(pl.multiple_of(HALF * n, 16), HALF)
        wg[at, :] = both[:HALF]
        wu[at, :] = both[HALF:]
        ends = mm(last[ALL], g[n, :, FF + D :]).astype(BF)
        ends = jnp.concatenate([ends[32 * t : 32 * t + 32] for t in range(7)], 1)
        packed = jnp.concatenate([g[n, :, FF : FF + D], ends], 0)
        wd[pl.ds(pl.multiple_of(288 * n, 16), 288), :] = mm(down[ALL], packed).astype(BF)
        return 0

    lax.fori_loop(0, 8, body, 0)


WEIGHTS = [pltpu.VMEM((D, FF), BF), pltpu.VMEM((D, FF), BF), pltpu.VMEM((FF, D), BF)]


def forward_kernel(x, g, *rest):
    picked, (_, h, a_out, slope_out, soft_out, s_out, gathered), rest = rest[:3], rest[3:10], rest[10:]
    saved, s, (wg, wu, wd), save_sem, sems = rest[:3], rest[3], rest[4:7], rest[7], rest[8:]
    gather = Gather(colours(C), None, gathered, *sems)
    tick = Ticks(gather, gather.steps((("begin", 2),) + LATE), GATHER_AT, 4)
    saves = [pltpu.make_async_copy(w, out, save_sem.at[n]) for n, (w, out) in enumerate(zip((wg, wu, wd), saved))]

    @pl.when(step_number() == 0)
    def _():
        unpack_all(g, picked, wg, wu, wd)
        for save in saves:
            save.start()

    tick(0)
    wide, scale = norm(x[ALL])
    a = (wide * scale).astype(BF)
    a_out[ALL] = a.T
    for n, at in enumerate(CHUNKS):
        gate, up = mm(a, wg[:, at]), mm(a, wu[:, at])
        soft, slope = gated(gate, up)
        slope_out[:, at] = slope
        soft_out[:, at] = soft
        s[:, at] = (soft * up).astype(BF)
        s_out[at, :] = s[:, at].T
        if n < 2:
            tick(n + 1)
    h[ALL] = (x[ALL].astype(F32) + mm(s[ALL], wd[ALL]).astype(BF).astype(F32)).astype(BF)
    tick(3)

    @pl.when(step_number() == 7)
    def _():
        for save in saves:
            save.wait()


def forward(x, g, part):
    n = TOK // 8
    return pl.pallas_call(
        forward_kernel,
        grid=(8,),
        in_specs=[rows(n, D), whole(PACKED), *PICKS, ANY],
        out_specs=[rows(n, D), columns(D, n), rows(n, FF), rows(n, FF), columns(FF, n), ANY, ANY, ANY, ANY],
        out_shape=[
            like(TOK, D), like(D, TOK), like(TOK, FF, F32), like(TOK, FF, F32), like(FF, TOK),
            jax.ShapeDtypeStruct(part.shape, BF), like(D, FF), like(D, FF), like(FF, D),
        ],
        scratch_shapes=[pltpu.VMEM((n, FF), BF), *WEIGHTS, pltpu.SemaphoreType.DMA((3,)), *GATHER_SEMS],
        input_output_aliases={5: 5},
        compiler_params=params(collective_id=2),
        name="forward",
    )(x, g.reshape(PACKED), *picks(), part)


def middle_kernel(h, dy, slope0, soft0, wd0, g, gu, down, last, a_out, s_out, dg_out, du_out, dh, dg0, du0, wg, wu, wd):
    @pl.when(step_number() == 0)
    def _():
        unpack_all(g, (gu, down, last), wg, wu, wd)

    wide, scale = norm(h[ALL])
    a = (wide * scale).astype(BF)
    a_out[ALL] = a.T
    for at in CHUNKS:
        gate, up = mm(a, wg[:, at]), mm(a, wu[:, at])
        ds = mmt(dy[ALL], wd[at, :]).astype(BF).astype(F32)
        soft, slope = gated(gate, up)
        s_out[at, :] = (soft * up).astype(BF).T
        dg_out[:, at] = (ds * slope).astype(BF)
        du_out[:, at] = (ds * soft).astype(BF)
    da = mmt(dg_out[ALL], wg[ALL]) + mmt(du_out[ALL], wu[ALL])
    by_h = norm_back(wide, scale, da, dy[ALL])
    dh[ALL] = by_h
    for at in CHUNKS:
        ds = mmt(by_h, wd0[at, :]).astype(BF).astype(F32)
        dg0[:, at] = (ds * slope0[:, at]).astype(BF)
        du0[:, at] = (ds * soft0[:, at]).astype(BF)


def middle(h, dy, slope, soft, wd, g):
    n = TOK // 8
    token, wide = rows(n, D), rows(n, FF)
    return pl.pallas_call(
        middle_kernel,
        grid=(8,),
        in_specs=[token, token, wide, wide, whole((FF, D)), whole(PACKED), *PICKS],
        out_specs=[columns(D, n), columns(FF, n), wide, wide, token, wide, wide],
        out_shape=[like(D, TOK), like(FF, TOK), like(TOK, FF), like(TOK, FF), like(TOK, D), like(TOK, FF), like(TOK, FF)],
        scratch_shapes=WEIGHTS,
        compiler_params=params(),
        name="middle",
    )(h, dy, slope, soft, wd, g.reshape(PACKED), *picks())


WIDE = 256
DOWN = 4
UP = FF // WIDE


def early(i):
    return jnp.minimum(i, DOWN - 1)


def late(i):
    return jnp.maximum(i - DOWN, 0)


def down_step(st, dy, down, last, out):
    w = mm(st[ALL], dy[ALL]).astype(BF)
    for n in range(2):
        packed = mm(down[ALL], w[288 * n : 288 * n + 288]).astype(BF)
        out[n, :, :D] = packed[:256]
        ends = jnp.concatenate([packed[256:, 128 * t : 128 * t + 128] for t in range(7)], 0)
        out[n, :, D:] = mm(last[ALL], ends).astype(BF)


def gate_up_step(at, dg, du, gu, out):
    wg = mm(at[ALL], dg[ALL]).astype(BF)
    wu = mm(at[ALL], du[ALL]).astype(BF)
    for n in range(8):
        cut = slice(HALF * n, HALF * n + HALF)
        out[n] = mm(gu[ALL], jnp.concatenate([wg[cut], wu[cut]], 0)).astype(BF)


DOWN_IN = [pl.BlockSpec((576, TOK), lambda i: (early(i), 0)), whole((TOK, D)), whole((288, 288)), whole((256, 224))]
DOWN_OUT = pl.BlockSpec((2, 256, 1024), lambda i: (early(i), 0, 0))


def by_packed(width):
    return jax.ShapeDtypeStruct((8, 256, width), BF)


def split(packed):
    return packed.reshape(*GRID, packed.shape[-1])


SUMMED = whole(POINT)


def weights_kernel(st, dy, down, last, at, dg, du, gu, *rest, reduce):
    tick = lambda slot: None
    if reduce:
        *before, down_out, gu_out, rounded, kept = rest[:6]
        scatter = scatter_first(before, rounded, kept, rest[6:])
        tick = Ticks(scatter, scatter.steps_first(), FIRST_AT, 2)
    else:
        down_out, gu_out = rest
    tick(0)
    pl.when(step_number() < DOWN)(lambda: down_step(st, dy, down, last, down_out))
    pl.when(step_number() >= DOWN)(lambda: gate_up_step(at, dg, du, gu, gu_out))
    tick(1)


def by_weights(st, dy, at, dg, du, before=()):
    gu, down, last = picks()
    tile = pl.BlockSpec((TOK, WIDE), lambda i: (0, late(i)))
    more = bool(before)
    by_down, by_gu, *out = pl.pallas_call(
        functools.partial(weights_kernel, reduce=more),
        grid=(DOWN + UP,),
        in_specs=[*DOWN_IN, whole((D, TOK)), tile, tile, whole((256, 224)), *[ANY for _ in before]],
        out_specs=[DOWN_OUT, pl.BlockSpec((8, 256, WIDE), lambda i: (0, 0, late(i))), *[whole(PLANE), whole(LINE)] * more],
        out_shape=[by_packed(1024), by_packed(FF), *[jax.ShapeDtypeStruct(PLANE, BF), jax.ShapeDtypeStruct(LINE, F32)] * more],
        scratch_shapes=FIRST * more,
        compiler_params=params(**(dict(collective_id=4) if more else {})),
        name="by_weights",
    )(st, dy, down.T, last.T, at, dg, du, gu.T, *before)
    return split(by_gu), split(by_down), *out


def backward_kernel(x, dh, dg, du, wg, wu, by_gu, by_down, rounded, kept, dx, out0, out1, *scratch):
    ahead = scatter_rest(scratch[0], kept, out1, scratch[1 : 1 + len(REST)])
    scatter = scatter_of((by_gu, by_down), out0, scratch[1 + len(REST) :])

    def resume():
        scratch[0][ALL] = rounded[ALL]
        others[0]()

    steps, others = scatter.steps(), ahead.steps_rest()
    mixed = [t for pair in zip(steps, [resume, *others[1:-1]]) for t in pair]
    tick = Ticks(scatter, [*mixed, *steps[len(others) - 1 :], others[-1]], BOTH_AT, 2)
    tick(0)
    wide, scale = norm(x[ALL])
    da = mmt(dg[ALL], wg[ALL]) + mmt(du[ALL], wu[ALL])
    dx[ALL] = norm_back(wide, scale, da, dh[ALL])
    tick(1)


def backward(x, dh, dg, du, wg, wu, before):
    n = TOK // 8
    return pl.pallas_call(
        backward_kernel,
        grid=(8,),
        in_specs=[
            rows(n, D), rows(n, D), rows(n, FF), rows(n, FF), whole((D, FF)), whole((D, FF)), ANY, ANY, whole(PLANE), whole(LINE),
        ],
        out_specs=[rows(n, D), SUMMED, SUMMED],
        out_shape=[like(TOK, D), like(*POINT), like(*POINT)],
        scratch_shapes=[pltpu.VMEM(PLANE, BF), *REST, *WHOLE],
        compiler_params=params(collective_id=3),
        name="backward",
    )(x, dh, dg, du, wg, wu, *before)


def solution(mesh):
    def step(x, dy, gate, up, down):
        x, dy = x[0], dy[0]
        part0, part1 = gather_call(*[pack_shard(gate[n], up[n], down[n]) for n in range(2)])
        h, a0, slope, soft, s0, part1, wg, wu, wd = forward(x, part0, part1)
        a1, s1, dg1, du1, dh, dg, du = middle(h, dy, slope, soft, wd, part1)
        before = by_weights(s1, dy, a1, dg1, du1)
        before = by_weights(s0, dh, a0, dg, du, before)
        dx, sum0, sum1 = backward(x, dh, dg, du, wg, wu, before)
        outs = [unpack_shard(t) for t in (sum0, sum1)]
        return (dx[None], *(jnp.stack([o[i] for o in outs]) for i in range(3)))

    cut = P(None, "dp", None)
    return jax.shard_map(
        step, mesh=mesh, in_specs=(P("dp"), P("dp"), cut, cut, cut), out_specs=(P("dp"), cut, cut, cut), check_vma=False
    )
```
